256 devices in a mesh: cfg: 2 (over y_hi), seq: 16 (over z, core), tp: 8 (over y_lo, x).
Axes of the slice: x: 4, y: 4 (y_hi: 2, y_lo: 2; y = y_hi * 2 + y_lo), z: 8, core: 2. Of those that a mesh axis runs over, the one named last changes fastest.
Arguments:
- queries: bfloat16 [2, 7680, 5120], P('cfg', 'seq', 'tp'), may hold values from -5 to 5
- keys: bfloat16 [2, 7680, 5120], P('cfg', 'seq', 'tp'), may hold values from -5 to 5
- values: bfloat16 [2, 7680, 5120], P('cfg', 'seq', 'tp'), may hold values from -5 to 5
- text_keys: bfloat16 [2, 512, 5120], P('cfg', None, 'tp'), may hold values from -7.5 to 7.5
- text_values: bfloat16 [2, 512, 5120], P('cfg', None, 'tp'), may hold values from -5 to 5
- prompt_lengths: int32 [2], P('cfg'), may hold values from 64 to 512
- frame_counts: int32 [16], P('seq'), may hold values from 240 to 480
- out_weight: bfloat16 [5120, 5120], P('tp'), may hold values from -0.5 to 0.5
Outputs:
- velocity: bfloat16 [7680, 5120], P('seq', ('tp', 'cfg'))
The draws below stay inside these ranges and needn't reach their ends.
All inputs are finite; a program needn't handle non-finite values.
Results may differ from the reference program's by a relative error of at most 0.015.
Values may be sent and summed in bfloat16 or wider, within the bound.
A program may use at most 256 MiB of HBM per device.

```python
import jax
import jax.numpy as jnp
from jax import lax

HEADS = 40
HEAD_DIM = 128
D = 5120
TEXT = 512
FRAME_SLOTS = 480
FRAMES = 16
TOKENS = 7680


def query_key_pair(key):
    base = jax.random.fold_in(key, 7)
    shape = (2, TOKENS, D)
    query_draw = jnp.clip(1.5 * jax.random.normal(jax.random.fold_in(base, 1), shape, jnp.float32), -5.0, 5.0)
    key_draw = jnp.clip(jax.random.normal(jax.random.fold_in(base, 2), shape, jnp.float32), -5.0, 5.0)
    return (query_draw, key_draw)


def draw_queries(key, part):
    return query_key_pair(key)[0].astype(jnp.bfloat16)


def draw_keys(key, part):
    return query_key_pair(key)[1].astype(jnp.bfloat16)


def touch_ends(entries, key, least, top_value):
    longest = entries.shape.index(max(entries.shape))
    spots = []
    for shift in (0, 1):
        where = [jax.random.randint(jax.random.fold_in(key, axis), (), 0, length) for axis, length in enumerate(entries.shape)]
        where[longest] = (where[longest] + shift) % entries.shape[longest]
        spots.append(tuple(where))
    return entries.at[spots[0]].set(least).at[spots[1]].set(top_value)


def levels(rng, shape, shards, smallest, high):
    def one(position, blocks):
        draws = jax.random.uniform(jax.random.fold_in(jax.random.fold_in(rng, 6), position), (blocks,), jnp.float32, smallest / len(shards), high / len(shards))
        return jnp.repeat(jnp.exp(draws), shape[position] // blocks).reshape((-1,) + (1,) * (len(shape) - position - 1))

    gain = one(*shards[0])
    for cut in shards[1:]:
        gain = gain * one(*cut)
    return gain


def normal_values(stream_key, extent, scale, limit, shards=(), kind=jnp.bfloat16):
    level = levels(stream_key, extent, shards, -0.22, 0.18) if shards else 1.0
    array = jax.random.normal(stream_key, extent, jnp.float32) * scale * level
    return jnp.minimum(jnp.maximum(array, -limit), limit).astype(kind)


def setup_inputs(seed: int = 0) -> dict:
    seeds = jax.random.split(jax.random.key(seed), 9)
    return {
        "queries": draw_queries(jax.random.fold_in(seeds[8], 71), 0),
        "keys": draw_keys(jax.random.fold_in(seeds[8], 71), 0),
        "values": normal_values(seeds[2], (2, TOKENS, D), 1.0, 5.0, ((0, 2), (1, 16), (2, 8))),
        "text_keys": normal_values(seeds[3], (2, TEXT, D), 1.5, 7.5, ((0, 2), (2, 8))),
        "text_values": normal_values(seeds[4], (2, TEXT, D), 1.0, 5.0, ((0, 2), (2, 8))),
        "prompt_lengths": jax.random.randint(seeds[5], (2,), TEXT // 8, TEXT + 1).astype(jnp.int32),
        "frame_counts": touch_ends(jax.random.randint(seeds[6], (FRAMES,), FRAME_SLOTS // 2, FRAME_SLOTS + 1), jax.random.fold_in(seeds[6], 1), FRAME_SLOTS // 2, FRAME_SLOTS).astype(jnp.int32),
        "out_weight": normal_values(seeds[7], (D, D), (D // 32) ** -0.5, 0.5, ((0, 8),)),
    }


GUIDANCE = 5.0
RESCALE = 0.7
NEGATIVE = -1e+30

def video_valid(frame_counts):
    positions = jnp.arange(TOKENS, dtype=jnp.int32)
    return positions % FRAME_SLOTS < frame_counts[positions // FRAME_SLOTS]

def branch_output(query_rows, key_rows, value_rows, text_key_rows, text_value_rows, length, video_mask, out_weight):
    text_mask = jnp.arange(TEXT, dtype=jnp.int32) < length
    full_mask = jnp.concatenate([text_mask, video_mask])
    all_keys = jnp.concatenate([text_key_rows, key_rows], axis=0)
    all_values = jnp.concatenate([text_value_rows, value_rows], axis=0)
    key_total = all_keys.shape[0]
    query_heads = jnp.transpose(query_rows.reshape(TOKENS, HEADS, HEAD_DIM), (1, 0, 2))
    key_heads = jnp.transpose(all_keys.reshape(key_total, HEADS, HEAD_DIM), (1, 0, 2))
    value_heads = jnp.transpose(all_values.reshape(key_total, HEADS, HEAD_DIM), (1, 0, 2))

    def one_head(operands):
        query_head, key_head, value_head = operands
        scores = jnp.dot(query_head, key_head.T, preferred_element_type=jnp.float32) * HEAD_DIM ** (-0.5)
        scores = jnp.where(full_mask[None, :], scores, NEGATIVE)
        row_max = lax.optimization_barrier(jnp.max(scores, axis=1, keepdims=True))
        weights = jnp.exp(scores - row_max)
        weight_sum = lax.optimization_barrier(jnp.sum(weights, axis=1, keepdims=True))
        mixed_rows = jnp.dot(weights.astype(jnp.bfloat16), value_head, preferred_element_type=jnp.float32)
        return (mixed_rows / weight_sum).astype(jnp.bfloat16)
    heads_out = lax.map(one_head, (query_heads, key_heads, value_heads))
    attended = jnp.transpose(heads_out, (1, 0, 2)).reshape(TOKENS, HEADS * HEAD_DIM)
    return jnp.dot(attended, out_weight, preferred_element_type=jnp.float32).astype(jnp.bfloat16)

def reference(queries, keys, values, text_keys, text_values, prompt_lengths, frame_counts, out_weight):
    video_mask = video_valid(frame_counts)
    conditional = branch_output(queries[0], keys[0], values[0], text_keys[0], text_values[0], prompt_lengths[0], video_mask, out_weight).astype(jnp.float32)
    unconditional = branch_output(queries[1], keys[1], values[1], text_keys[1], text_values[1], prompt_lengths[1], video_mask, out_weight).astype(jnp.float32)
    guided = unconditional + GUIDANCE * (conditional - unconditional)
    token_weights = video_mask.astype(jnp.float32)
    valid_total = jnp.sum(frame_counts).astype(jnp.float32)

    def moment(field_rows):
        return jnp.dot(token_weights, field_rows, precision=lax.Precision.HIGHEST) / valid_total
    guided_mean = moment(guided)
    guided_var = moment(guided * guided) - guided_mean * guided_mean
    cond_mean = moment(conditional)
    cond_var = moment(conditional * conditional) - cond_mean * cond_mean
    std_ratio = jnp.sqrt((cond_var + 1.0) / (guided_var + 1.0))
    factor = RESCALE * std_ratio + (1.0 - RESCALE)
    return (guided_mean + (guided - guided_mean) * factor).astype(jnp.bfloat16)
```

```python
import functools

import jax
import jax.numpy as jnp
from jax import lax
from jax.experimental import pallas as pl
from jax.experimental.pallas import tpu as pltpu
from jax.sharding import PartitionSpec as P

MESH = pl.DeviceIdType.MESH
HD = 128
GUIDANCE = 5.0
RESCALE = 0.7
NEGATIVE = -1e30
LOG2E = 1.4426950408889634
F32 = jnp.float32
BF16 = jnp.bfloat16


def kernel(
    dims,
    plen_ref, count_ref, cnt_in, q_ref, k_ref, v_ref, tk_ref, tv_ref, w_hbm,
    out_ref,
    kbuf, vbuf, valid, tkbuf, tvbuf, tvalid, cbuf, m_ref, acc, obuf, wbuf,
    oacc, mine, give, got, stat, statbuf,
    ring_send, ring_recv, d2d_send, d2d_recv, cnt_send, cnt_recv,
    o_send, o_recv, w_send, w_recv, wd_send, wd_recv, w_loc,
    x_send, x_recv, st_send, st_recv,
):
    heads, rows, trows, nseq, ntp, cols = dims
    nz = nseq // 2
    half = rows // 2
    wide = out_ref.shape[1] + 64
    scale = HD ** (-0.5) * LOG2E
    me = lax.axis_index("seq")
    tp = lax.axis_index("tp")
    cfg = lax.axis_index("cfg")
    z = me // 2
    core = lax.rem(me, 2)
    up = lax.rem(z + 1, nz) * 2 + core
    down = lax.rem(z + nz - 1, nz) * 2 + core
    mate = z * 2 + (1 - core)
    count = count_ref[0]
    plen = plen_ref[0]

    def remote(src, dst, ss, rs, **to):
        return pltpu.make_async_remote_copy(
            src_ref=src, dst_ref=dst, send_sem=ss, recv_sem=rs,
            device_id=to, device_id_type=MESH,
        )

    row_id = lax.broadcasted_iota(jnp.int32, (rows, HD), 0)
    trow_id = lax.broadcasted_iota(jnp.int32, (trows, HD), 0)
    for h in range(heads):
        cut = slice(h * HD, (h + 1) * HD)
        kk = k_ref[:, cut].astype(F32)
        vv = v_ref[:, cut].astype(F32)
        kbuf[h, 0:rows, :] = jnp.where(row_id < count, kk, kk[0:1, :]).astype(BF16)
        vbuf[h, 0:rows, :] = jnp.where(row_id < count, vv, 0.0).astype(BF16)

    barrier = pltpu.get_barrier_semaphore()
    for d in range(1, nseq):
        pl.semaphore_signal(barrier, inc=1, device_id={"seq": lax.rem(me + d, nseq)}, device_id_type=MESH)
    for d in range(1, ntp):
        pl.semaphore_signal(barrier, inc=1, device_id={"tp": lax.rem(tp + d, ntp)}, device_id_type=MESH)
    pl.semaphore_signal(barrier, inc=1, device_id={"cfg": 1 - cfg}, device_id_type=MESH)
    pl.semaphore_wait(barrier, nseq - 1 + ntp - 1 + 1)

    def slot(kind, s):
        if s == 4:
            return 14
        return 2 + 4 * (s - 1) + (0 if kind < 2 else 2)

    def buf_of(kind):
        return kbuf if kind % 2 == 0 else vbuf

    def at(kind, h, sl):
        return buf_of(kind).at[h, pl.ds(sl * rows, rows), :]

    def last(kind):
        return 4 if kind in (0, 3) else 3

    def ring(h, kind, s):
        src = at(kind, h, 0 if s == 1 else slot(kind, s - 1))
        return remote(src, at(kind, h, slot(kind, s)), ring_send.at[h, kind, s - 1],
                      ring_recv.at[h, kind, s - 1], seq=(up if kind < 2 else down))

    def d2d_index(kind, s):
        if s == 0:
            return 0
        if s == 4:
            return 7
        return s if kind < 2 else 3 + s

    def d2d(h, kind, s):
        sl = 0 if s == 0 else slot(kind, s)
        i = d2d_index(kind, s)
        return remote(at(kind, h, sl), at(kind, h, sl + 1), d2d_send.at[h, kind % 2, i],
                      d2d_recv.at[h, kind % 2, i], seq=mate)

    def launch(h):
        for kind in (0, 2, 1, 3):
            ring(h, kind, 1).start()
        d2d(h, 0, 0).start()
        d2d(h, 1, 0).start()

    def pass_on(h, kind, s):
        if s > last(kind):
            return
        ring(h, kind, s).wait_recv()
        if s < last(kind):
            ring(h, kind, s + 1).start()
        d2d(h, kind, s).start()

    def cnt(d):
        peer = lax.rem(me + d, nseq)
        return remote(cnt_in, cbuf.at[me], cnt_send.at[d], cnt_recv.at[d], seq=peer)

    def wcopy(d):
        peer = lax.rem(tp + d, ntp)
        return remote(
            w_hbm.at[:, pl.ds(core * 64, 64), pl.ds(pl.multiple_of(peer * cols, HD), cols)],
            wbuf.at[:, pl.ds(tp * HD + core * 64, 64), :],
            w_send.at[d], w_recv.at[d], tp=peer)

    def wmate(d):
        src = lax.rem(tp + ntp - d, ntp)
        part = wbuf.at[:, pl.ds(src * HD + core * 64, 64), :]
        return remote(part, part, wd_send.at[d], wd_recv.at[d], seq=mate)

    def ocopy(h, d):
        peer = lax.rem(tp + d, ntp)
        return remote(obuf.at[h, tp], obuf.at[h, tp], o_send.at[h, d], o_recv.at[h, d], tp=peer)

    for d in range(1, nseq):
        cnt(d).start()
    launch(0)
    own_w = pltpu.make_async_copy(
        w_hbm.at[:, :, pl.ds(pl.multiple_of(tp * cols, HD), cols)],
        wbuf.at[:, pl.ds(tp * HD, HD), :], w_loc)
    own_w.start()
    for d in range(1, ntp):
        wcopy(d).start()

    for h in range(heads):
        cut = slice(h * HD, (h + 1) * HD)
        kk = tk_ref[:, cut].astype(F32)
        vv = tv_ref[:, cut].astype(F32)
        tkbuf[h] = jnp.where(trow_id < plen, kk, kk[0:1, :]).astype(BF16)
        tvbuf[h] = jnp.where(trow_id < plen, vv, 0.0).astype(BF16)
    tvalid[...] = jnp.where(trow_id < plen, 1.0, 0.0).astype(BF16)

    cbuf[me] = jnp.broadcast_to(count.astype(F32), cbuf.shape[1:])
    for d in range(1, nseq):
        cnt(d).wait_recv()
    for sl in range(nseq):
        if sl < 2:
            zz, other = z, sl
        elif sl >= 14:
            zz, other = lax.rem(z + 4, nz), sl - 14
        else:
            s, r = 1 + (sl - 2) // 4, (sl - 2) % 4
            zz = lax.rem(z + nz - s, nz) if r < 2 else lax.rem(z + s, nz)
            other = r % 2
        src = zz * 2 + (core if other == 0 else 1 - core)
        c = cbuf[src][0:1, :]
        valid[sl * rows:(sl + 1) * rows, :] = jnp.where(row_id.astype(F32) < c, 1.0, 0.0).astype(BF16)

    def spread(x, n):
        full, rest = divmod(n, HD)
        parts = [x] * full + ([x[:, :rest]] if rest else [])
        return parts[0] if len(parts) == 1 else jnp.concatenate(parts, axis=1)

    def attend(h, part, k, v, ok, first=False):
        r = pl.ds(part * half, half)
        q = q_ref[r, pl.ds(pl.multiple_of(h * HD, HD), HD)]
        s = lax.dot_general(q, k, (((1,), (1,)), ((), ())), preferred_element_type=F32)
        n = s.shape[1]
        mb = jnp.max(s, axis=1, keepdims=True) * scale
        if first:
            m_new = jnp.broadcast_to(mb, (half, HD))
        else:
            m_old = m_ref[r, :]
            m_new = jnp.maximum(m_old, mb)
        p = jnp.exp2(s * scale - spread(m_new, n)).astype(BF16)
        pv = lax.dot_general(p, jnp.concatenate([v, ok], axis=1), (((1,), (0,)), ((), ())),
                             preferred_element_type=F32)
        if first:
            acc[r, :] = pv
        else:
            shrink = jnp.exp2(m_old - m_new)
            acc[r, :] = acc[r, :] * jnp.concatenate([shrink, shrink], axis=1) + pv
        m_ref[r, :] = m_new

    def attend_slots(h, part, sl, n):
        r = pl.ds(sl * rows, n * rows)
        attend(h, part, kbuf[h, r, :], vbuf[h, r, :], valid[r, :])

    def project(h, first=False):
        lhs = jnp.concatenate([obuf[h, j] for j in range(ntp)], axis=1)
        res = jnp.dot(lhs, wbuf[h], preferred_element_type=F32)
        if first:
            oacc[...] = res
        else:
            oacc[...] += res

    oacc[...] = jnp.zeros_like(oacc)

    def head_step(h, _):
        for part in range(2):
            attend(h, part, tkbuf[h], tvbuf[h], tvalid[...], first=True)

        @pl.when(h == 2)
        def _():
            for d in range(1, ntp):
                wcopy(d).wait_recv()
                wmate(d).start()

        for s in range(1, 5):
            pass_on(h, 0, s)
            pass_on(h, 2, s)
            if s == 1:
                d2d(h, 0, 0).wait_recv()
                d2d(h, 1, 0).wait_recv()
                attend_slots(h, 0, 0, 2)
            else:
                for kind in range(4):
                    d2d(h, kind, s - 1).wait_recv()
                attend_slots(h, 0, 2 + 4 * (s - 2), 4)
            pass_on(h, 1, s)
            pass_on(h, 3, s)
            if s == 3:
                @pl.when(h < heads - 1)
                def _():
                    launch(h + 1)
            if s == 1:
                attend_slots(h, 1, 0, 2)
            else:
                attend_slots(h, 1, 2 + 4 * (s - 2), 4)
            if s == 3:
                @pl.when(h == 2)
                def _():
                    own_w.wait()
                    for d in range(1, ntp):
                        wmate(d).wait_recv()

                @pl.when(h >= 2)
                def _():
                    for d in range(1, ntp):
                        ocopy(h - 2, d).wait_recv()
                    project(h - 2)
        d2d(h, 0, 4).wait_recv()
        d2d(h, 3, 4).wait_recv()
        for part in range(2):
            attend_slots(h, part, 14, 2)
            r = pl.ds(part * half, half)
            obuf[h, tp, r, :] = (acc[r, 0:HD] / acc[r, HD:2 * HD]).astype(BF16)
        for d in range(1, ntp):
            ocopy(h, d).start()
        return 0

    lax.fori_loop(0, heads, head_step, 0)

    for h in (heads - 2, heads - 1):
        for d in range(1, ntp):
            ocopy(h, d).wait_recv()
        project(h)

    out = oacc[...]
    low, high = out[:, 0:wide], out[:, cols - wide:]
    mine[...] = jnp.where(cfg == 0, low, high).astype(BF16)
    give[...] = jnp.where(cfg == 0, high, low).astype(BF16)
    swap = remote(give, got, x_send, x_recv, cfg=1 - cfg)
    swap.start()
    swap.wait_recv()

    a = mine[...].astype(F32)
    b = got[...].astype(F32)
    cond = jnp.where(cfg == 0, a, b)
    uncond = jnp.where(cfg == 0, b, a)
    guided = uncond + GUIDANCE * (cond - uncond)
    live = lax.broadcasted_iota(jnp.int32, (rows, wide), 0) < count
    gl = jnp.where(live, guided, 0.0)
    cl = jnp.where(live, cond, 0.0)
    sums = [jnp.sum(t, axis=0, keepdims=True) for t in (gl, gl * gl, cl, cl * cl)]
    stat[...] = jnp.concatenate(sums + [jnp.zeros((4, wide), F32)], axis=0)
    statbuf[me] = stat[...]

    def st(d):
        return remote(stat, statbuf.at[me], st_send.at[d], st_recv.at[d], seq=lax.rem(me + d, nseq))

    for d in range(1, nseq):
        st(d).start()
    for d in range(1, nseq):
        st(d).wait_recv()
    total = statbuf[0]
    number = cbuf[0][0:1, :]
    for i in range(1, nseq):
        total = total + statbuf[i]
        number = number + cbuf[i][0:1, :]
    number = spread(number, wide)
    g_mean = total[0:1] / number
    g_var = total[1:2] / number - g_mean * g_mean
    c_mean = total[2:3] / number
    c_var = total[3:4] / number - c_mean * c_mean
    factor = RESCALE * jnp.sqrt((c_var + 1.0) / (g_var + 1.0)) + (1.0 - RESCALE)
    vel = g_mean + (guided - g_mean) * factor
    keep = wide - 64
    out_ref[...] = jnp.where(cfg == 0, vel[:, :keep], vel[:, 64:]).astype(BF16)

    def drain(h, _):
        for kind in range(4):
            for s in range(1, last(kind) + 1):
                ring(h, kind, s).wait_send()
            for s in range(0 if kind < 2 else 1, last(kind) + 1):
                d2d(h, kind, s).wait_send()
        for d in range(1, ntp):
            ocopy(h, d).wait_send()
        return 0

    lax.fori_loop(0, heads, drain, 0)
    for d in range(1, nseq):
        cnt(d).wait_send()
        st(d).wait_send()
    for d in range(1, ntp):
        wcopy(d).wait_send()
        wmate(d).wait_send()
    swap.wait_send()


def body(queries, keys, values, text_keys, text_values, prompt_lengths, frame_counts, out_weight):
    rows, width = queries.shape[1:]
    trows = text_keys.shape[1]
    heads = width // HD
    nseq, ntp = lax.axis_size("seq"), lax.axis_size("tp")
    model = out_weight.shape[1]
    cols = model // ntp
    keep = cols // 2
    wide = keep + 64
    cnt_tile = jnp.broadcast_to(frame_counts.astype(F32), (8, HD))
    vm = pl.BlockSpec(memory_space=pltpu.VMEM)
    sm = pl.BlockSpec(memory_space=pltpu.SMEM)
    hbm = pl.BlockSpec(memory_space=pl.ANY)
    dma = pltpu.SemaphoreType.DMA
    return pl.pallas_call(
        functools.partial(kernel, (heads, rows, trows, nseq, ntp, cols)),
        out_shape=jax.ShapeDtypeStruct((rows, keep), BF16),
        in_specs=[sm, sm, vm, vm, vm, vm, vm, vm, hbm],
        out_specs=vm,
        scratch_shapes=[
            pltpu.VMEM((heads, nseq * rows, HD), BF16),
            pltpu.VMEM((heads, nseq * rows, HD), BF16),
            pltpu.VMEM((nseq * rows, HD), BF16),
            pltpu.VMEM((heads, trows, HD), BF16),
            pltpu.VMEM((heads, trows, HD), BF16),
            pltpu.VMEM((trows, HD), BF16),
            pltpu.VMEM((nseq, 8, HD), F32),
            pltpu.VMEM((rows, HD), F32),
            pltpu.VMEM((rows, 2 * HD), F32),
            pltpu.VMEM((heads, ntp, rows, HD), BF16),
            pltpu.VMEM((heads, ntp * HD, cols), BF16),
            pltpu.VMEM((rows, cols), F32),
            pltpu.VMEM((rows, wide), BF16),
            pltpu.VMEM((rows, wide), BF16),
            pltpu.VMEM((rows, wide), BF16),
            pltpu.VMEM((8, wide), F32),
            pltpu.VMEM((nseq, 8, wide), F32),
            dma((heads, 4, 4)), dma((heads, 4, 4)),
            dma((heads, 2, 8)), dma((heads, 2, 8)),
            dma((nseq,)), dma((nseq,)),
            dma((heads, ntp)), dma((heads, ntp)),
            dma((ntp,)), dma((ntp,)), dma((ntp,)), dma((ntp,)), dma,
            dma, dma, dma((nseq,)), dma((nseq,)),
        ],
        compiler_params=pltpu.CompilerParams(
            collective_id=0, has_side_effects=True, vmem_limit_bytes=60 * 1024 * 1024
        ),
    )(
        prompt_lengths, frame_counts, cnt_tile, queries[0], keys[0], values[0],
        text_keys[0], text_values[0], out_weight.reshape(heads, HD, model),
    )


def solution(mesh):
    placed = (
        P("cfg", "seq", "tp"),
        P("cfg", "seq", "tp"),
        P("cfg", "seq", "tp"),
        P("cfg", None, "tp"),
        P("cfg", None, "tp"),
        P("cfg"),
        P("seq"),
        P("tp", None),
    )
    return jax.shard_map(
        body, mesh=mesh, in_specs=placed, out_specs=P("seq", ("tp", "cfg")), check_vma=False
    )
```

```python
import functools

import jax
import jax.numpy as jnp
from jax import lax
from jax.experimental import pallas as pl
from jax.experimental.pallas import tpu as pltpu
from jax.sharding import PartitionSpec as P

MESH = pl.DeviceIdType.MESH
HD = 128
GUIDANCE = 5.0
RESCALE = 0.7
NEGATIVE = -1e30
LOG2E = 1.4426950408889634
F32 = jnp.float32
BF16 = jnp.bfloat16


def kernel(
    dims,
    plen_ref, count_ref, q_hbm, k_hbm, v_hbm, tk_hbm, tv_hbm, w_hbm,
    out_ref,
    q_ref, k_ref, v_ref, tk_ref, tv_ref, cnt_in,
    kbuf, vbuf, valid, tkbuf, tvbuf, tvalid, cbuf, m_ref, acc, obuf, wbuf,
    oacc, stat, statbuf,
    ring_send, ring_recv, d2d_send, d2d_recv, cnt_send, cnt_recv,
    o_send, o_recv, w_send, w_recv, wd_send, wd_recv, w_loc, in_sem,
    st_send, st_recv,
):
    heads, rows, trows, nseq, ntp, cols = dims
    nz = nseq // 2
    half = rows // 2
    wide = out_ref.shape[1] + 64
    scale = HD ** (-0.5) * LOG2E
    me = lax.axis_index("seq")
    tp = lax.axis_index("tp")
    cfg = lax.axis_index("cfg")
    z = me // 2
    core = lax.rem(me, 2)
    up = lax.rem(z + 1, nz) * 2 + core
    down = lax.rem(z + nz - 1, nz) * 2 + core
    mate = z * 2 + (1 - core)
    nplane = 2 * ntp
    spot = cfg * ntp + tp
    side = 4
    step_a = jnp.where(core == 0, 1, side)
    step_b = jnp.where(core == 0, side, 1)
    pa = lax.rem(spot // step_a, side)
    pb = lax.rem(spot // step_b, side)

    def place(da, db):
        return lax.rem(pa + da + side, side) * step_a + lax.rem(pb + db + side, side) * step_b

    count = count_ref[0]
    plen = plen_ref[0]

    def remote(src, dst, ss, rs, **to):
        return pltpu.make_async_remote_copy(
            src_ref=src, dst_ref=dst, send_sem=ss, recv_sem=rs,
            device_id=to, device_id_type=MESH,
        )

    barrier = pltpu.get_barrier_semaphore()
    for d in range(1, nseq):
        pl.semaphore_signal(barrier, inc=1, device_id={"seq": lax.rem(me + d, nseq)}, device_id_type=MESH)
    for d in range(1, nplane):
        peer = lax.rem(spot + d, nplane)
        pl.semaphore_signal(barrier, inc=1, device_id={"cfg": peer // ntp, "tp": lax.rem(peer, ntp)},
                            device_id_type=MESH)
    loads = [pltpu.make_async_copy(a, b, in_sem.at[i]) for i, (a, b) in enumerate(
        ((k_hbm, k_ref), (v_hbm, v_ref), (tk_hbm, tk_ref), (tv_hbm, tv_ref), (q_hbm, q_ref)))]
    for copy in loads:
        copy.start()
    cnt_in[...] = jnp.broadcast_to(count.astype(F32), cnt_in.shape)
    loads[0].wait()
    loads[1].wait()

    row_id = lax.broadcasted_iota(jnp.int32, (rows, HD), 0)
    trow_id = lax.broadcasted_iota(jnp.int32, (trows, HD), 0)
    scope = jax.named_scope
    for h in range(heads):
        cut = slice(h * HD, (h + 1) * HD)
        kk = k_ref[:, cut].astype(F32)
        vv = v_ref[:, cut].astype(F32)
        kbuf[h, 0:rows, :] = jnp.where(row_id < count, kk, kk[0:1, :]).astype(BF16)
        vbuf[h, 0:rows, :] = jnp.where(row_id < count, vv, 0.0).astype(BF16)

    with scope("entry"):
        pl.semaphore_wait(barrier, nseq - 1 + nplane - 1)

    def slot(kind, s):
        if s == 4:
            return 14
        return 2 + 4 * (s - 1) + (0 if kind < 2 else 2)

    def buf_of(kind):
        return kbuf if kind % 2 == 0 else vbuf

    def at(kind, h, sl):
        return buf_of(kind).at[h, pl.ds(sl * rows, rows), :]

    def last(kind):
        return 4 if kind in (0, 3) else 3

    def ring(h, kind, s):
        src = at(kind, h, 0 if s == 1 else slot(kind, s - 1))
        return remote(src, at(kind, h, slot(kind, s)), ring_send,
                      ring_recv.at[lax.rem(h, 2), kind, s - 1], seq=(up if kind < 2 else down))

    def d2d_index(kind, s):
        if s == 0:
            return 0
        if s == 4:
            return 7
        return s if kind < 2 else 3 + s

    def d2d(h, kind, s):
        sl = 0 if s == 0 else slot(kind, s)
        i = d2d_index(kind, s)
        return remote(at(kind, h, sl), at(kind, h, sl + 1), d2d_send,
                      d2d_recv.at[lax.rem(h, 2), kind % 2, i], seq=mate)

    def launch(h):
        for kind in (0, 2, 1, 3):
            ring(h, kind, 1).start()
        d2d(h, 0, 0).start()
        d2d(h, 1, 0).start()

    def pass_on(h, kind, s):
        if s > last(kind):
            return
        ring(h, kind, s).wait_recv()
        if s < last(kind):
            ring(h, kind, s + 1).start()
        d2d(h, kind, s).start()

    def cnt(d):
        peer = lax.rem(me + d, nseq)
        return remote(cnt_in, cbuf.at[me], cnt_send, cnt_recv, seq=peer)

    def window(owner):
        return pl.ds(pl.multiple_of(owner * cols + cfg * (cols - wide), HD), wide)

    def wcopy(d):
        peer = lax.rem(tp + d, ntp)
        return remote(
            w_hbm.at[:, pl.ds(core * 64, 64), window(peer)],
            wbuf.at[:, pl.ds(tp * HD + core * 64, 64), :],
            w_send, w_recv, tp=peer)

    def wmate(d):
        src = lax.rem(tp + ntp - d, ntp)
        part = wbuf.at[:, pl.ds(src * HD + core * 64, 64), :]
        return remote(part, part, wd_send, wd_recv, seq=mate)

    def bytes_of(ref, sem):
        pltpu.make_async_copy(ref, ref, sem).wait()

    upper, lower = slice(0, half), slice(half, rows)

    def hand(h, da, db, ta, tb, stage, r=None):
        part = obuf.at[h, place(da, db)]
        if r is not None:
            part = obuf.at[h, place(da, db), r, :]
        peer = place(ta, tb)
        remote(part, part, o_send, o_recv.at[h, stage],
               cfg=peer // ntp, tp=lax.rem(peer, ntp)).start()

    def blocks(h, stage, n):
        bytes_of(obuf.at[h, 0:n], o_recv.at[h, stage])

    def relay(h, stage):
        if stage == 0:
            for d in (1, -1):
                hand(h, 0, 0, d, 0, 0)
            for d in (1, -1):
                hand(h, 0, 0, 0, d, 2)
        elif stage == 1:
            blocks(h, 0, 2)
            hand(h, -1, 0, 1, 0, 1, upper)
            hand(h, 1, 0, -1, 0, 1, lower)
            for a in (-1, 1):
                for d in (1, -1):
                    hand(h, a, 0, 0, d, 3)
        elif stage == 2:
            blocks(h, 1, 1)
            for d in (1, -1):
                hand(h, 2, 0, 0, d, 4)
            blocks(h, 2, 2)
            hand(h, 0, -1, 0, 1, 5, upper)
            hand(h, 0, 1, 0, -1, 5, lower)
        elif stage == 3:
            blocks(h, 3, 4)
            for a in (-1, 1):
                hand(h, a, -1, 0, 1, 5, upper)
                hand(h, a, 1, 0, -1, 5, lower)
            blocks(h, 4, 2)
            hand(h, 2, -1, 0, 1, 5, upper)
            hand(h, 2, 1, 0, -1, 5, lower)
        else:
            blocks(h, 5, 4)

    launch(0)
    for d in range(1, nseq):
        cnt(d).start()
    own_w = pltpu.make_async_copy(
        w_hbm.at[:, :, window(tp)],
        wbuf.at[:, pl.ds(tp * HD, HD), :], w_loc)
    own_w.start()
    for d in range(1, ntp):
        wcopy(d).start()

    loads[2].wait()
    loads[3].wait()
    loads[4].wait()
    for h in range(heads):
        cut = slice(h * HD, (h + 1) * HD)
        kk = tk_ref[:, cut].astype(F32)
        vv = tv_ref[:, cut].astype(F32)
        tkbuf[h] = jnp.where(trow_id < plen, kk, kk[0:1, :]).astype(BF16)
        tvbuf[h] = jnp.where(trow_id < plen, vv, 0.0).astype(BF16)
    tvalid[...] = jnp.where(trow_id < plen, 1.0, 0.0).astype(BF16)

    cbuf[me] = jnp.broadcast_to(count.astype(F32), cbuf.shape[1:])
    with scope("first_k"):
        pass_on(0, 0, 1)
        pass_on(0, 2, 1)
    def mark(sl):
        if sl < 2:
            zz, other = z, sl
        elif sl >= 14:
            zz, other = lax.rem(z + 4, nz), sl - 14
        else:
            s, r = 1 + (sl - 2) // 4, (sl - 2) % 4
            zz = lax.rem(z + nz - s, nz) if r < 2 else lax.rem(z + s, nz)
            other = r % 2
        src = zz * 2 + (core if other == 0 else 1 - core)
        c = cbuf[src][0:1, :]
        valid[sl * rows:(sl + 1) * rows, :] = jnp.where(row_id.astype(F32) < c, 1.0, 0.0).astype(BF16)

    def spread(x, n):
        full, rest = divmod(n, HD)
        parts = [x] * full + ([x[:, :rest]] if rest else [])
        return parts[0] if len(parts) == 1 else jnp.concatenate(parts, axis=1)

    def attend(h, part, k, v, ok, first=False):
        r = pl.ds(part * half, half)
        now = lax.rem(h, 2)
        q = q_ref[r, pl.ds(pl.multiple_of(h * HD, HD), HD)]
        s = lax.dot_general(q, k, (((1,), (1,)), ((), ())), preferred_element_type=F32)
        n = s.shape[1]
        mb = jnp.max(s, axis=1, keepdims=True) * scale
        if first:
            m_new = jnp.broadcast_to(mb, (half, HD))
        else:
            m_old = m_ref[now, r, :]
            m_new = jnp.maximum(m_old, mb)
        p = jnp.exp2(s * scale - spread(m_new, n)).astype(BF16)
        pv = lax.dot_general(p, jnp.concatenate([v, ok], axis=1), (((1,), (0,)), ((), ())),
                             preferred_element_type=F32)
        if first:
            acc[now, r, :] = pv
        else:
            shrink = jnp.exp2(m_old - m_new)
            acc[now, r, :] = acc[now, r, :] * jnp.concatenate([shrink, shrink], axis=1) + pv
        m_ref[now, r, :] = m_new

    def attend_slots(h, part, sl, n):
        r = pl.ds(sl * rows, n * rows)
        attend(h, part, kbuf[h, r, :], vbuf[h, r, :], valid[r, :])

    def attend_text(h):
        for part in range(2):
            attend(h, part, tkbuf[h], tvbuf[h], tvalid[...], first=True)

    def project(h):
        for c in range(2):
            lhs = jnp.concatenate([obuf[h, c * ntp + j] for j in range(ntp)], axis=1)
            oacc[c] += jnp.dot(lhs, wbuf[h], preferred_element_type=F32)

    oacc[...] = jnp.zeros_like(oacc)

    attend_text(0)
    with scope("first_v"):
        pass_on(0, 1, 1)
        pass_on(0, 3, 1)
    with scope("counts"):
        bytes_of(cbuf.at[0:nseq - 1], cnt_recv)
    mark(0)
    mark(1)
    d2d(0, 0, 0).wait_recv()
    d2d(0, 1, 0).wait_recv()
    attend_slots(0, 0, 0, 2)

    def head_step(h, _):
        def note(group):
            @pl.when(h == 0)
            def _():
                for sl in range(2 + 4 * group, min(6 + 4 * group, nseq)):
                    mark(sl)

        def k_in(s):
            with scope(f"wk{s}"):
                pass_on(h, 0, s)
                pass_on(h, 2, s)

        def v_in(s):
            with scope(f"wv{s}"):
                pass_on(h, 1, s)
                pass_on(h, 3, s)

        def d_in(s):
            with scope(f"wd{s}"):
                for kind in range(4):
                    if s <= last(kind) and (s < 4 or kind in (0, 3)):
                        d2d(h, kind, s).wait_recv()

        k_in(2)
        attend_slots(h, 1, 0, 2)
        d_in(1)
        note(0)
        attend_slots(h, 0, 2, 4)
        v_in(2)

        @pl.when(h >= 1)
        def _():
            with scope("relay1"):
                relay(h - 1, 1)
        attend_slots(h, 1, 2, 4)

        @pl.when(h == 3)
        def _():
            with scope("ww2"):
                bytes_of(wbuf.at[:, 0:(ntp - 1) * 64, :], wd_recv)
                own_w.wait()

        @pl.when(h >= 3)
        def _():
            with scope("proj"):
                relay(h - 3, 4)
                project(h - 3)
        k_in(3)
        d_in(2)
        note(1)
        attend_slots(h, 0, 6, 4)
        v_in(3)

        @pl.when(h < heads - 1)
        def _():
            launch(h + 1)

        @pl.when(h >= 1)
        def _():
            with scope("relay2"):
                relay(h - 1, 2)
        attend_slots(h, 1, 6, 4)
        d_in(3)
        note(2)
        attend_slots(h, 0, 10, 4)
        k_in(4)
        v_in(4)

        @pl.when(h == 2)
        def _():
            with scope("ww"):
                bytes_of(wbuf.at[:, 0:(ntp - 1) * 64, :], w_recv)
                for d in range(1, ntp):
                    wmate(d).start()

        attend_slots(h, 1, 10, 4)

        @pl.when(h >= 1)
        def _():
            with scope("relay3"):
                relay(h - 1, 3)

        @pl.when(h < heads - 1)
        def _():
            with scope("wk1"):
                pass_on(h + 1, 0, 1)
                pass_on(h + 1, 2, 1)
            attend_text(h + 1)
            d2d(h + 1, 0, 0).wait_recv()
            d2d(h + 1, 1, 0).wait_recv()
            attend_slots(h + 1, 0, 0, 2)
            with scope("wv1"):
                pass_on(h + 1, 1, 1)
                pass_on(h + 1, 3, 1)
        d_in(4)
        note(3)
        now = lax.rem(h, 2)
        for part in range(2):
            attend_slots(h, part, 14, 2)
            r = pl.ds(part * half, half)
            obuf[h, spot, r, :] = (acc[now, r, 0:HD] / acc[now, r, HD:2 * HD]).astype(BF16)
        relay(h, 0)
        return 0

    lax.fori_loop(0, heads, head_step, 0)

    with scope("last1"):
        relay(heads - 1, 1)
    for h in (heads - 3, heads - 2):
        with scope(f"late{h}"):
            relay(h, 4)
        project(h)
    for stage in range(2, 5):
        with scope(f"last{stage}"):
            relay(heads - 1, stage)
    project(heads - 1)

    cond = oacc[0].astype(BF16).astype(F32)
    uncond = oacc[1].astype(BF16).astype(F32)
    guided = uncond + GUIDANCE * (cond - uncond)
    live = lax.broadcasted_iota(jnp.int32, (rows, wide), 0) < count
    gl = jnp.where(live, guided, 0.0)
    cl = jnp.where(live, cond, 0.0)
    sums = [jnp.sum(t, axis=0, keepdims=True) for t in (gl, gl * gl, cl, cl * cl)]
    tiles = wide // HD
    lines = [t[:, i * HD:(i + 1) * HD] for t in sums for i in range(tiles)]
    stat[...] = jnp.concatenate(lines + [jnp.zeros((16 - 4 * tiles, HD), F32)], axis=0)
    statbuf[me] = stat[...]

    def st(d):
        return remote(stat, statbuf.at[me], st_send, st_recv, seq=lax.rem(me + d, nseq))

    for d in range(1, nseq):
        st(d).start()
    with scope("stats"):
        bytes_of(statbuf.at[0:nseq - 1], st_recv)
    total = statbuf[0]
    number = cbuf[0][0:1, :]
    for i in range(1, nseq):
        total = total + statbuf[i]
        number = number + cbuf[i][0:1, :]
    number = spread(number, wide)
    g_sum, g_square, c_sum, c_square = (
        jnp.concatenate([total[j * tiles + i:j * tiles + i + 1] for i in range(tiles)], axis=1)
        for j in range(4))
    g_mean = g_sum / number
    g_var = g_square / number - g_mean * g_mean
    c_mean = c_sum / number
    c_var = c_square / number - c_mean * c_mean
    factor = RESCALE * jnp.sqrt((c_var + 1.0) / (g_var + 1.0)) + (1.0 - RESCALE)
    vel = g_mean + (guided - g_mean) * factor
    keep = wide - 64
    out_ref[...] = jnp.where(cfg == 0, vel[:, :keep], vel[:, 64:]).astype(BF16)

    with scope("drain"):
        bytes_of(kbuf.at[:, 0:14 * rows, :], ring_send)
        bytes_of(kbuf, d2d_send)
        bytes_of(obuf.at[:, 0:nplane - 1], o_send)
        bytes_of(cbuf.at[0:nseq - 1], cnt_send)
        bytes_of(statbuf.at[0:nseq - 1], st_send)
        bytes_of(wbuf.at[:, 0:(ntp - 1) * 64, :], w_send)
        bytes_of(wbuf.at[:, 0:(ntp - 1) * 64, :], wd_send)


def body(queries, keys, values, text_keys, text_values, prompt_lengths, frame_counts, out_weight):
    rows, width = queries.shape[1:]
    trows = text_keys.shape[1]
    heads = width // HD
    nseq, ntp = lax.axis_size("seq"), lax.axis_size("tp")
    model = out_weight.shape[1]
    cols = model // ntp
    keep = cols // 2
    wide = keep + 64
    vm = pl.BlockSpec(memory_space=pltpu.VMEM)
    sm = pl.BlockSpec(memory_space=pltpu.SMEM)
    hbm = pl.BlockSpec(memory_space=pl.ANY)
    dma = pltpu.SemaphoreType.DMA
    return pl.pallas_call(
        functools.partial(kernel, (heads, rows, trows, nseq, ntp, cols)),
        out_shape=jax.ShapeDtypeStruct((rows, keep), BF16),
        in_specs=[sm, sm, hbm, hbm, hbm, hbm, hbm, hbm],
        out_specs=vm,
        scratch_shapes=[
            pltpu.VMEM((rows, width), BF16),
            pltpu.VMEM((rows, width), BF16),
            pltpu.VMEM((rows, width), BF16),
            pltpu.VMEM((trows, width), BF16),
            pltpu.VMEM((trows, width), BF16),
            pltpu.VMEM((8, HD), F32),
            pltpu.VMEM((heads, nseq * rows, HD), BF16),
            pltpu.VMEM((heads, nseq * rows, HD), BF16),
            pltpu.VMEM((nseq * rows, HD), BF16),
            pltpu.VMEM((heads, trows, HD), BF16),
            pltpu.VMEM((heads, trows, HD), BF16),
            pltpu.VMEM((trows, HD), BF16),
            pltpu.VMEM((nseq, 8, HD), F32),
            pltpu.VMEM((2, rows, HD), F32),
            pltpu.VMEM((2, rows, 2 * HD), F32),
            pltpu.VMEM((heads, 2 * ntp, rows, HD), BF16),
            pltpu.VMEM((heads, ntp * HD, wide), BF16),
            pltpu.VMEM((2, rows, wide), F32),
            pltpu.VMEM((16, HD), F32),
            pltpu.VMEM((nseq, 16, HD), F32),
            dma, dma((2, 4, 4)), dma, dma((2, 2, 8)), dma, dma,
            dma, dma((heads, 6)), dma, dma, dma, dma, dma, dma((5,)),
            dma, dma,
        ],
        compiler_params=pltpu.CompilerParams(
            collective_id=0, has_side_effects=True, vmem_limit_bytes=60 * 1024 * 1024
        ),
    )(
        prompt_lengths, frame_counts, queries[0], keys[0], values[0],
        text_keys[0], text_values[0], out_weight.reshape(heads, HD, model),
    )


def solution(mesh):
    placed = (
        P("cfg", "seq", "tp"),
        P("cfg", "seq", "tp"),
        P("cfg", "seq", "tp"),
        P("cfg", None, "tp"),
        P("cfg", None, "tp"),
        P("cfg"),
        P("seq"),
        P("tp", None),
    )
    return jax.shard_map(
        body, mesh=mesh, in_specs=placed, out_specs=P("seq", ("tp", "cfg")), check_vma=False
    )
```

```python
import functools

import jax
import jax.numpy as jnp
from jax import lax
from jax.experimental import pallas as pl
from jax.experimental.pallas import tpu as pltpu
from jax.sharding import PartitionSpec as P

MESH = pl.DeviceIdType.MESH
HD = 128
GUIDANCE = 5.0
RESCALE = 0.7
NEGATIVE = -1e30
LOG2E = 1.4426950408889634
F32 = jnp.float32
BF16 = jnp.bfloat16


def kernel(
    dims,
    plen_ref, count_ref, q_hbm, k_hbm, v_hbm, tk_hbm, tv_hbm, w_hbm,
    out_ref,
    q_ref, k_ref, v_ref, tk_ref, tv_ref, cnt_in,
    kbuf, vbuf, valid, tkbuf, tvbuf, tvalid, cbuf, m_ref, acc, obuf, wbuf,
    oacc, stat, statbuf,
    ring_send, ring_recv, d2d_send, d2d_recv, cnt_send, cnt_recv,
    o_send, o_recv, w_send, w_recv, wd_send, wd_recv, w_loc, in_sem,
    st_send, st_recv,
):
    heads, rows, trows, nseq, ntp, cols = dims
    nz = nseq // 2
    half = rows // 2
    wide = out_ref.shape[1] + 64
    scale = HD ** (-0.5) * LOG2E
    me = lax.axis_index("seq")
    tp = lax.axis_index("tp")
    cfg = lax.axis_index("cfg")
    z = me // 2
    core = lax.rem(me, 2)
    up = lax.rem(z + 1, nz) * 2 + core
    down = lax.rem(z + nz - 1, nz) * 2 + core
    mate = z * 2 + (1 - core)
    nplane = 2 * ntp
    spot = cfg * ntp + tp
    side = 4
    step_a = jnp.where(core == 0, 1, side)
    step_b = jnp.where(core == 0, side, 1)
    pa = lax.rem(spot // step_a, side)
    pb = lax.rem(spot // step_b, side)

    def place(da, db):
        return lax.rem(pa + da + side, side) * step_a + lax.rem(pb + db + side, side) * step_b

    count = count_ref[0]
    plen = plen_ref[0]

    def remote(src, dst, ss, rs, **to):
        return pltpu.make_async_remote_copy(
            src_ref=src, dst_ref=dst, send_sem=ss, recv_sem=rs,
            device_id=to, device_id_type=MESH,
        )

    barrier = pltpu.get_barrier_semaphore()
    for d in range(1, nseq):
        pl.semaphore_signal(barrier, inc=1, device_id={"seq": lax.rem(me + d, nseq)}, device_id_type=MESH)
    for d in range(1, nplane):
        peer = lax.rem(spot + d, nplane)
        pl.semaphore_signal(barrier, inc=1, device_id={"cfg": peer // ntp, "tp": lax.rem(peer, ntp)},
                            device_id_type=MESH)
    loads = [pltpu.make_async_copy(a, b, in_sem.at[i]) for i, (a, b) in enumerate(
        ((k_hbm, k_ref), (v_hbm, v_ref), (tk_hbm, tk_ref), (tv_hbm, tv_ref), (q_hbm, q_ref)))]
    for copy in loads:
        copy.start()
    cnt_in[...] = jnp.broadcast_to(count.astype(F32), cnt_in.shape)
    loads[0].wait()
    loads[1].wait()

    row_id = lax.broadcasted_iota(jnp.int32, (rows, HD), 0)
    trow_id = lax.broadcasted_iota(jnp.int32, (trows, HD), 0)
    scope = jax.named_scope
    for h in range(heads):
        cut = slice(h * HD, (h + 1) * HD)
        kk = k_ref[:, cut].astype(F32)
        vv = v_ref[:, cut].astype(F32)
        kbuf[h, 0:rows, :] = jnp.where(row_id < count, kk, kk[0:1, :]).astype(BF16)
        vbuf[h, 0:rows, :] = jnp.where(row_id < count, vv, 0.0).astype(BF16)

    with scope("entry"):
        pl.semaphore_wait(barrier, nseq - 1 + nplane - 1)

    def slot(kind, s):
        if s == 4:
            return 14
        return 2 + 4 * (s - 1) + (0 if kind < 2 else 2)

    def buf_of(kind):
        return kbuf if kind % 2 == 0 else vbuf

    def at(kind, h, sl):
        return buf_of(kind).at[h, pl.ds(sl * rows, rows), :]

    def last(kind):
        return 4 if kind in (0, 3) else 3

    def ring(h, kind, s):
        src = at(kind, h, 0 if s == 1 else slot(kind, s - 1))
        return remote(src, at(kind, h, slot(kind, s)), ring_send,
                      ring_recv.at[lax.rem(h, 2), kind, s - 1], seq=(up if kind < 2 else down))

    def d2d_index(kind, s):
        if s == 0:
            return 0
        if s == 4:
            return 7
        return s if kind < 2 else 3 + s

    def d2d(h, kind, s):
        sl = 0 if s == 0 else slot(kind, s)
        i = d2d_index(kind, s)
        return remote(at(kind, h, sl), at(kind, h, sl + 1), d2d_send,
                      d2d_recv.at[lax.rem(h, 2), kind % 2, i], seq=mate)

    def launch(h, ahead):
        if ahead:
            ring(h, 2, 1).start()
            return
        for kind in (0, 1, 3):
            ring(h, kind, 1).start()
        d2d(h, 0, 0).start()
        d2d(h, 1, 0).start()

    def pass_on(h, kind, s):
        if s > last(kind):
            return
        ring(h, kind, s).wait_recv()
        if s < last(kind):
            ring(h, kind, s + 1).start()
        d2d(h, kind, s).start()

    def cnt(d):
        peer = lax.rem(me + d, nseq)
        return remote(cnt_in.at[0:1, :], cbuf.at[me, 0:1, :], cnt_send, cnt_recv, seq=peer)

    def window(owner):
        return pl.ds(pl.multiple_of(owner * cols + cfg * (cols - wide), HD), wide)

    def wcopy(d):
        peer = lax.rem(tp + d, ntp)
        return remote(
            w_hbm.at[:, pl.ds(core * 64, 64), window(peer)],
            wbuf.at[:, pl.ds(tp * HD + core * 64, 64), :],
            w_send, w_recv, tp=peer)

    def wmate(d):
        src = lax.rem(tp + ntp - d, ntp)
        part = wbuf.at[:, pl.ds(src * HD + core * 64, 64), :]
        return remote(part, part, wd_send, wd_recv, seq=mate)

    def bytes_of(ref, sem):
        pltpu.make_async_copy(ref, ref, sem).wait()

    upper, lower = slice(0, half), slice(half, rows)

    def hand(h, da, db, ta, tb, stage, r=None):
        part = obuf.at[h, place(da, db)]
        if r is not None:
            part = obuf.at[h, place(da, db), r, :]
        peer = place(ta, tb)
        remote(part, part, o_send, o_recv.at[h, stage],
               cfg=peer // ntp, tp=lax.rem(peer, ntp)).start()

    def blocks(h, stage, n):
        bytes_of(obuf.at[h, 0:n], o_recv.at[h, stage])

    def relay(h, stage):
        if stage == 0:
            for d in (1, -1):
                hand(h, 0, 0, d, 0, 0)
            for d in (1, -1):
                hand(h, 0, 0, 0, d, 2)
        elif stage == 1:
            blocks(h, 0, 2)
            hand(h, -1, 0, 1, 0, 1, upper)
            hand(h, 1, 0, -1, 0, 1, lower)
            for a in (-1, 1):
                for d in (1, -1):
                    hand(h, a, 0, 0, d, 3)
            blocks(h, 2, 2)
            hand(h, 0, -1, 0, 1, 5, upper)
            hand(h, 0, 1, 0, -1, 5, lower)
        elif stage == 2:
            blocks(h, 1, 1)
            for d in (1, -1):
                hand(h, 2, 0, 0, d, 4)
        elif stage == 3:
            blocks(h, 3, 4)
            for a in (-1, 1):
                hand(h, a, -1, 0, 1, 5, upper)
                hand(h, a, 1, 0, -1, 5, lower)
            blocks(h, 4, 2)
            hand(h, 2, -1, 0, 1, 5, upper)
            hand(h, 2, 1, 0, -1, 5, lower)
        else:
            blocks(h, 5, 4)

    for d in range(1, nseq):
        cnt(d).start()
    launch(0, True)
    launch(0, False)
    own_w = pltpu.make_async_copy(
        w_hbm.at[:, :, window(tp)],
        wbuf.at[:, pl.ds(tp * HD, HD), :], w_loc)
    own_w.start()
    for d in range(1, ntp):
        wcopy(d).start()

    loads[2].wait()
    loads[3].wait()
    loads[4].wait()
    for h in range(heads):
        cut = slice(h * HD, (h + 1) * HD)
        kk = tk_ref[:, cut].astype(F32)
        vv = tv_ref[:, cut].astype(F32)
        tkbuf[h] = jnp.where(trow_id < plen, kk, kk[0:1, :]).astype(BF16)
        tvbuf[h] = jnp.where(trow_id < plen, vv, 0.0).astype(BF16)
    tvalid[...] = jnp.where(trow_id < plen, 1.0, 0.0).astype(BF16)

    cbuf[me] = jnp.broadcast_to(count.astype(F32), cbuf.shape[1:])
    with scope("first_k"):
        pass_on(0, 0, 1)
        pass_on(0, 2, 1)
    def mark(sl):
        if sl < 2:
            zz, other = z, sl
        elif sl >= 14:
            zz, other = lax.rem(z + 4, nz), sl - 14
        else:
            s, r = 1 + (sl - 2) // 4, (sl - 2) % 4
            zz = lax.rem(z + nz - s, nz) if r < 2 else lax.rem(z + s, nz)
            other = r % 2
        src = zz * 2 + (core if other == 0 else 1 - core)
        c = cbuf[src][0:1, :]
        valid[sl * rows:(sl + 1) * rows, :] = jnp.where(row_id.astype(F32) < c, 1.0, 0.0).astype(BF16)

    def spread(x, n):
        full, rest = divmod(n, HD)
        parts = [x] * full + ([x[:, :rest]] if rest else [])
        return parts[0] if len(parts) == 1 else jnp.concatenate(parts, axis=1)

    def attend(h, part, k, v, ok, first=False):
        r = pl.ds(part * half, half)
        now = lax.rem(h, 2)
        q = q_ref[r, pl.ds(pl.multiple_of(h * HD, HD), HD)]
        s = lax.dot_general(q, k, (((1,), (1,)), ((), ())), preferred_element_type=F32)
        n = s.shape[1]
        mb = jnp.max(s, axis=1, keepdims=True) * scale
        if first:
            m_new = jnp.broadcast_to(mb, (half, HD))
        else:
            m_old = m_ref[now, r, :]
            m_new = jnp.maximum(m_old, mb)
        p = jnp.exp2(s * scale - spread(m_new, n)).astype(BF16)
        pv = lax.dot_general(p, jnp.concatenate([v, ok], axis=1), (((1,), (0,)), ((), ())),
                             preferred_element_type=F32)
        if first:
            acc[now, r, :] = pv
        else:
            shrink = jnp.exp2(m_old - m_new)
            acc[now, r, :] = acc[now, r, :] * jnp.concatenate([shrink, shrink], axis=1) + pv
        m_ref[now, r, :] = m_new

    def attend_slots(h, part, sl, n):
        r = pl.ds(sl * rows, n * rows)
        attend(h, part, kbuf[h, r, :], vbuf[h, r, :], valid[r, :])

    def attend_text(h):
        for part in range(2):
            attend(h, part, tkbuf[h], tvbuf[h], tvalid[...], first=True)

    def project(h):
        for c in range(2):
            lhs = jnp.concatenate([obuf[h, c * ntp + j] for j in range(ntp)], axis=1)
            oacc[c] += jnp.dot(lhs, wbuf[h], preferred_element_type=F32)

    oacc[...] = jnp.zeros_like(oacc)

    attend_text(0)
    with scope("first_v"):
        pass_on(0, 1, 1)
        pass_on(0, 3, 1)
    with scope("counts"):
        bytes_of(cbuf.at[0:nseq - 1, 0:1, :], cnt_recv)
    mark(0)
    mark(1)
    d2d(0, 0, 0).wait_recv()
    d2d(0, 1, 0).wait_recv()
    attend_slots(0, 0, 0, 2)

    def head_step(h, _):
        def note(group):
            @pl.when(h == 0)
            def _():
                for sl in range(2 + 4 * group, min(6 + 4 * group, nseq)):
                    mark(sl)

        def k_in(s):
            with scope(f"wk{s}"):
                pass_on(h, 0, s)
                if s < 4:
                    pass_on(h, 2, s)

        def v_in(s):
            with scope(f"wv{s}"):
                pass_on(h, 1, s)
                pass_on(h, 3, s)

        def d_in(s):
            with scope(f"wd{s}"):
                for kind in range(4):
                    if s <= last(kind) and (s < 4 or kind in (0, 3)):
                        d2d(h, kind, s).wait_recv()

        k_in(2)
        attend_slots(h, 1, 0, 2)
        d_in(1)
        note(0)
        attend_slots(h, 0, 2, 4)
        v_in(2)

        @pl.when(h >= 1)
        def _():
            with scope("relay1"):
                relay(h - 1, 1)
        attend_slots(h, 1, 2, 4)

        @pl.when(h == 2)
        def _():
            with scope("ww2"):
                bytes_of(wbuf.at[:, 0:(ntp - 1) * 64, :], wd_recv)
                own_w.wait()

        @pl.when(h >= 2)
        def _():
            with scope("proj"):
                relay(h - 2, 4)
                project(h - 2)
        k_in(3)

        @pl.when(h < heads - 1)
        def _():
            launch(h + 1, True)
        d_in(2)
        note(1)
        attend_slots(h, 0, 6, 4)
        v_in(3)

        @pl.when(h < heads - 1)
        def _():
            launch(h + 1, False)

        @pl.when(h >= 1)
        def _():
            with scope("relay2"):
                relay(h - 1, 2)
        attend_slots(h, 1, 6, 4)
        d_in(3)
        note(2)
        attend_slots(h, 0, 10, 4)
        k_in(4)

        @pl.when(h < heads - 1)
        def _():
            with scope("wk1d"):
                pass_on(h + 1, 2, 1)

        @pl.when(h == heads - 1)
        def _():
            with scope("wv4"):
                pass_on(h, 3, 4)

        @pl.when(h == 1)
        def _():
            with scope("ww"):
                bytes_of(wbuf.at[:, 0:(ntp - 1) * 64, :], w_recv)
                for d in range(1, ntp):
                    wmate(d).start()

        attend_slots(h, 1, 10, 4)

        @pl.when(h >= 1)
        def _():
            with scope("relay3"):
                relay(h - 1, 3)

        @pl.when(h < heads - 1)
        def _():
            with scope("wk1"):
                pass_on(h + 1, 0, 1)
                pass_on(h, 3, 4)
            attend_text(h + 1)
            d2d(h + 1, 0, 0).wait_recv()
            d2d(h + 1, 1, 0).wait_recv()
            attend_slots(h + 1, 0, 0, 2)
            with scope("wv1"):
                pass_on(h + 1, 1, 1)
                pass_on(h + 1, 3, 1)
        d_in(4)
        note(3)
        now = lax.rem(h, 2)
        for part in range(2):
            attend_slots(h, part, 14, 2)
            r = pl.ds(part * half, half)
            obuf[h, spot, r, :] = (acc[now, r, 0:HD] / acc[now, r, HD:2 * HD]).astype(BF16)
        relay(h, 0)
        return 0

    lax.fori_loop(0, heads, head_step, 0)

    with scope("last1"):
        relay(heads - 1, 1)
    with scope("late"):
        relay(heads - 2, 4)
    project(heads - 2)
    for stage in range(2, 5):
        with scope(f"last{stage}"):
            relay(heads - 1, stage)
    project(heads - 1)

    cond = oacc[0].astype(BF16).astype(F32)
    uncond = oacc[1].astype(BF16).astype(F32)
    guided = uncond + GUIDANCE * (cond - uncond)
    live = lax.broadcasted_iota(jnp.int32, (rows, wide), 0) < count
    gl = jnp.where(live, guided, 0.0)
    cl = jnp.where(live, cond, 0.0)
    sums = [jnp.sum(t, axis=0, keepdims=True) for t in (gl, gl * gl, cl, cl * cl)]
    tiles = wide // HD
    lines = [t[:, i * HD:(i + 1) * HD] for t in sums for i in range(tiles)]
    stat[...] = jnp.concatenate(lines + [jnp.zeros((16 - 4 * tiles, HD), F32)], axis=0)
    statbuf[me] = stat[...]

    def st(d):
        return remote(stat, statbuf.at[me], st_send, st_recv, seq=lax.rem(me + d, nseq))

    for d in range(1, nseq):
        st(d).start()
    with scope("stats"):
        bytes_of(statbuf.at[0:nseq - 1], st_recv)
    total = statbuf[0]
    number = cbuf[0][0:1, :]
    for i in range(1, nseq):
        total = total + statbuf[i]
        number = number + cbuf[i][0:1, :]
    number = spread(number, wide)
    g_sum, g_square, c_sum, c_square = (
        jnp.concatenate([total[j * tiles + i:j * tiles + i + 1] for i in range(tiles)], axis=1)
        for j in range(4))
    g_mean = g_sum / number
    g_var = g_square / number - g_mean * g_mean
    c_mean = c_sum / number
    c_var = c_square / number - c_mean * c_mean
    factor = RESCALE * jnp.sqrt((c_var + 1.0) / (g_var + 1.0)) + (1.0 - RESCALE)
    vel = g_mean + (guided - g_mean) * factor
    keep = wide - 64
    out_ref[...] = jnp.where(cfg == 0, vel[:, :keep], vel[:, 64:]).astype(BF16)

    with scope("drain"):
        bytes_of(kbuf.at[:, 0:14 * rows, :], ring_send)
        bytes_of(kbuf, d2d_send)
        bytes_of(obuf.at[:, 0:nplane - 1], o_send)
        bytes_of(cbuf.at[0:nseq - 1, 0:1, :], cnt_send)
        bytes_of(statbuf.at[0:nseq - 1], st_send)
        bytes_of(wbuf.at[:, 0:(ntp - 1) * 64, :], w_send)
        bytes_of(wbuf.at[:, 0:(ntp - 1) * 64, :], wd_send)


def body(queries, keys, values, text_keys, text_values, prompt_lengths, frame_counts, out_weight):
    rows, width = queries.shape[1:]
    trows = text_keys.shape[1]
    heads = width // HD
    nseq, ntp = lax.axis_size("seq"), lax.axis_size("tp")
    model = out_weight.shape[1]
    cols = model // ntp
    keep = cols // 2
    wide = keep + 64
    vm = pl.BlockSpec(memory_space=pltpu.VMEM)
    sm = pl.BlockSpec(memory_space=pltpu.SMEM)
    hbm = pl.BlockSpec(memory_space=pl.ANY)
    dma = pltpu.SemaphoreType.DMA
    return pl.pallas_call(
        functools.partial(kernel, (heads, rows, trows, nseq, ntp, cols)),
        out_shape=jax.ShapeDtypeStruct((rows, keep), BF16),
        in_specs=[sm, sm, hbm, hbm, hbm, hbm, hbm, hbm],
        out_specs=vm,
        scratch_shapes=[
            pltpu.VMEM((rows, width), BF16),
            pltpu.VMEM((rows, width), BF16),
            pltpu.VMEM((rows, width), BF16),
            pltpu.VMEM((trows, width), BF16),
            pltpu.VMEM((trows, width), BF16),
            pltpu.VMEM((8, HD), F32),
            pltpu.VMEM((heads, nseq * rows, HD), BF16),
            pltpu.VMEM((heads, nseq * rows, HD), BF16),
            pltpu.VMEM((nseq * rows, HD), BF16),
            pltpu.VMEM((heads, trows, HD), BF16),
            pltpu.VMEM((heads, trows, HD), BF16),
            pltpu.VMEM((trows, HD), BF16),
            pltpu.VMEM((nseq, 8, HD), F32),
            pltpu.VMEM((2, rows, HD), F32),
            pltpu.VMEM((2, rows, 2 * HD), F32),
            pltpu.VMEM((heads, 2 * ntp, rows, HD), BF16),
            pltpu.VMEM((heads, ntp * HD, wide), BF16),
            pltpu.VMEM((2, rows, wide), F32),
            pltpu.VMEM((16, HD), F32),
            pltpu.VMEM((nseq, 16, HD), F32),
            dma, dma((2, 4, 4)), dma, dma((2, 2, 8)), dma, dma,
            dma, dma((heads, 6)), dma, dma, dma, dma, dma, dma((5,)),
            dma, dma,
        ],
        compiler_params=pltpu.CompilerParams(
            collective_id=0, has_side_effects=True, vmem_limit_bytes=60 * 1024 * 1024
        ),
    )(
        prompt_lengths, frame_counts, queries[0], keys[0], values[0],
        text_keys[0], text_values[0], out_weight.reshape(heads, HD, model),
    )


def solution(mesh):
    placed = (
        P("cfg", "seq", "tp"),
        P("cfg", "seq", "tp"),
        P("cfg", "seq", "tp"),
        P("cfg", None, "tp"),
        P("cfg", None, "tp"),
        P("cfg"),
        P("seq"),
        P("tp", None),
    )
    return jax.shard_map(
        body, mesh=mesh, in_specs=placed, out_specs=P("seq", ("tp", "cfg")), check_vma=False
    )
```

```python
import functools

import jax
import jax.numpy as jnp
from jax import lax
from jax.experimental import pallas as pl
from jax.experimental.pallas import tpu as pltpu
from jax.sharding import PartitionSpec as P

MESH = pl.DeviceIdType.MESH
HD = 128
GUIDANCE = 5.0
RESCALE = 0.7
NEGATIVE = -1e30
LOG2E = 1.4426950408889634
F32 = jnp.float32
BF16 = jnp.bfloat16


def kernel(
    dims,
    plen_ref, count_ref, q_hbm, k_hbm, v_hbm, tk_hbm, tv_hbm, w_hbm,
    out_ref,
    k_ref, v_ref, tk_ref, tv_ref, cnt_in, qout, kvout, qhome, qring,
    kvh, kvr, valid_h, valid_r, tkv, tvalid, cbuf, m_ref, acc, oback, obuf, wbuf,
    oacc, stat, statbuf,
    q_send, q_recv, kv_send, kv_recv, kb_recv, kd_send, kd_recv, kbd_recv,
    ring_send, ring_recv, d2d_send, d2d_recv, cnt_send, cnt_recv, back_send, back_recv,
    o_send, o_recv, w_send, w_recv, wd_send, wd_recv, w_loc, in_sem,
    st_send, st_recv,
):
    heads, rows, trows, nseq, ntp, cols = dims
    nz = nseq // 2
    units = 4
    half = rows // 2
    wide = out_ref.shape[1] + 64
    scale = HD ** (-0.5) * LOG2E
    me = lax.axis_index("seq")
    tp = lax.axis_index("tp")
    cfg = lax.axis_index("cfg")
    z = me // 2
    core = lax.rem(me, 2)
    odd = lax.rem(z, 2)
    up = lax.rem(z + 1, nz) * 2 + core
    down = lax.rem(z + nz - 1, nz) * 2 + core
    mate = z * 2 + (1 - core)
    buddy = (z + 1 - 2 * odd) * 2 + core
    nplane = 2 * ntp
    spot = cfg * ntp + tp
    side = 4
    step_a = jnp.where(core == 0, 1, side)
    step_b = jnp.where(core == 0, side, 1)
    pa = lax.rem(spot // step_a, side)
    pb = lax.rem(spot // step_b, side)

    def place(da, db):
        return lax.rem(pa + da + side, side) * step_a + lax.rem(pb + db + side, side) * step_b

    def target(u):
        flip = lax.rem(odd + u, 2)
        return lax.rem(z + nz + u * (1 - 2 * flip), nz)

    def owner(u):
        return lax.rem(z + nz + u * (2 * odd - 1), nz)

    def other_owner(u):
        return lax.rem(z + nz - (1 + u) * (2 * odd - 1), nz)

    def head_of(u):
        return target(u) // 2 if u else z // 2

    def lanes(h):
        return pl.ds(pl.multiple_of(h * HD, HD), HD)

    count = count_ref[0]
    plen = plen_ref[0]
    scope = jax.named_scope

    def remote(src, dst, ss, rs, **to):
        return pltpu.make_async_remote_copy(
            src_ref=src, dst_ref=dst, send_sem=ss, recv_sem=rs,
            device_id=to, device_id_type=MESH,
        )

    def bytes_of(ref, sem):
        pltpu.make_async_copy(ref, ref, sem).wait()

    barrier = pltpu.get_barrier_semaphore()
    for d in range(1, nseq):
        pl.semaphore_signal(barrier, inc=1, device_id={"seq": lax.rem(me + d, nseq)}, device_id_type=MESH)
    for d in range(1, nplane):
        peer = lax.rem(spot + d, nplane)
        pl.semaphore_signal(barrier, inc=1, device_id={"cfg": peer // ntp, "tp": lax.rem(peer, ntp)},
                            device_id_type=MESH)
    pairs = [(k_hbm, k_ref), (v_hbm, v_ref), (tk_hbm, tk_ref), (tv_hbm, tv_ref),
             (q_hbm.at[:, lanes(head_of(0))], qhome.at[0]),
             (q_hbm.at[:, lanes(heads - 1)], qring)]
    pairs += [(q_hbm.at[:, lanes(head_of(u))], qout.at[u - 1]) for u in range(1, units)]
    loads = [pltpu.make_async_copy(a, b, in_sem.at[i]) for i, (a, b) in enumerate(pairs)]
    for copy in loads:
        copy.start()
    cnt_in[...] = jnp.broadcast_to(count.astype(F32), cnt_in.shape)
    loads[0].wait()
    loads[1].wait()

    row_id = lax.broadcasted_iota(jnp.int32, (rows, HD), 0)
    trow_id = lax.broadcasted_iota(jnp.int32, (trows, HD), 0)
    for u in range(units + 1):
        cut = lanes(head_of(u) if u < units else heads - 1)
        kk = k_ref[:, cut].astype(F32)
        vv = v_ref[:, cut].astype(F32)
        kk = jnp.where(row_id < count, kk, kk[0:1, :]).astype(BF16)
        vv = jnp.where(row_id < count, vv, 0.0).astype(BF16)
        if u == 0:
            kvh[0, 0:rows, :] = kk
            kvh[1, 0:rows, :] = vv
        elif u < units:
            kvout[u - 1, 0] = kk
            kvout[u - 1, 1] = vv
        else:
            kvr[0, 0:rows, :] = kk
            kvr[1, 0:rows, :] = vv
    for copy in loads[4:]:
        copy.wait()

    with scope("entry"):
        pl.semaphore_wait(barrier, nseq - 1 + nplane - 1)

    def hslot(i):
        return kvh.at[:, pl.ds(i * rows, rows), :]

    def q_out(u):
        return remote(qout.at[u - 1], qhome.at[u], q_send, q_recv.at[u - 1], seq=target(u) * 2 + core)

    def kv_out(u):
        return remote(kvout.at[u - 1], hslot(4 * u), kv_send, kv_recv.at[u - 1], seq=target(u) * 2 + core)

    def kv_buddy(u):
        return remote(hslot(4 * u), hslot(4 * u + 2), kv_send, kb_recv.at[u], seq=buddy)

    def kv_mate(u):
        return remote(hslot(4 * u), hslot(4 * u + 1), kd_send, kd_recv.at[u], seq=mate)

    def kv_buddy_mate(u):
        return remote(hslot(4 * u + 2), hslot(4 * u + 3), kd_send, kbd_recv.at[u], seq=mate)

    def o_back(u):
        return remote(oback.at[u - 1], obuf.at[u, spot], back_send, back_recv.at[u - 1], seq=owner(u) * 2 + core)

    def slot(kind, s):
        if s == 4:
            return 14
        return 2 + 4 * (s - 1) + (0 if kind < 2 else 2)

    def at(kind, sl):
        return kvr.at[kind % 2, pl.ds(sl * rows, rows), :]

    def last(kind):
        return 4 if kind in (0, 3) else 3

    def ring(kind, s):
        src = at(kind, 0 if s == 1 else slot(kind, s - 1))
        return remote(src, at(kind, slot(kind, s)), ring_send,
                      ring_recv.at[kind, s - 1], seq=(up if kind < 2 else down))

    def d2d(kind, s):
        sl = 0 if s == 0 else slot(kind, s)
        i = {0: 0, 4: 7}.get(s, s if kind < 2 else 3 + s)
        return remote(at(kind, sl), at(kind, sl + 1), d2d_send,
                      d2d_recv.at[kind % 2, i], seq=mate)

    def pass_on(kind, s):
        if s > last(kind):
            return
        ring(kind, s).wait_recv()
        if s < last(kind):
            ring(kind, s + 1).start()
        d2d(kind, s).start()

    def d_in(s):
        for kind in range(4):
            if s <= last(kind) and (s < 4 or kind in (0, 3)):
                d2d(kind, s).wait_recv()

    def cnt(d):
        peer = lax.rem(me + d, nseq)
        return remote(cnt_in.at[0:1, :], cbuf.at[me, 0:1, :], cnt_send, cnt_recv, seq=peer)

    def window(who):
        return pl.ds(pl.multiple_of(who * cols + cfg * (cols - wide), HD), wide)

    def wcopy(d):
        peer = lax.rem(tp + d, ntp)
        return remote(
            w_hbm.at[:, pl.ds(core * 64, 64), window(peer)],
            wbuf.at[:, pl.ds(tp * HD + core * 64, 64), :],
            w_send, w_recv, tp=peer)

    def wmate(d):
        src = lax.rem(tp + ntp - d, ntp)
        part = wbuf.at[:, pl.ds(src * HD + core * 64, 64), :]
        return remote(part, part, wd_send, wd_recv, seq=mate)

    upper, lower = slice(0, half), slice(half, rows)

    def hand(u, da, db, ta, tb, stage, r=None):
        part = obuf.at[u, place(da, db)]
        if r is not None:
            part = obuf.at[u, place(da, db), r, :]
        peer = place(ta, tb)
        remote(part, part, o_send, o_recv.at[u, stage],
               cfg=peer // ntp, tp=lax.rem(peer, ntp)).start()

    def blocks(u, stage, n):
        bytes_of(obuf.at[u, 0:n], o_recv.at[u, stage])

    def relay(u, stage):
        with scope(f"R{u}{stage}"):
            relay_step(u, stage)

    def relay_step(u, stage):
        if stage == 0:
            if 0 < u < units:
                o_back(u).wait_recv()
            for d in (1, -1):
                hand(u, 0, 0, d, 0, 0)
            for d in (1, -1):
                hand(u, 0, 0, 0, d, 2)
        elif stage == 1:
            blocks(u, 0, 2)
            hand(u, -1, 0, 1, 0, 1, upper)
            hand(u, 1, 0, -1, 0, 1, lower)
            for a in (-1, 1):
                for d in (1, -1):
                    hand(u, a, 0, 0, d, 3)
            blocks(u, 2, 2)
            hand(u, 0, -1, 0, 1, 5, upper)
            hand(u, 0, 1, 0, -1, 5, lower)
        elif stage == 2:
            blocks(u, 1, 1)
            for d in (1, -1):
                hand(u, 2, 0, 0, d, 4)
        elif stage == 3:
            blocks(u, 3, 4)
            for a in (-1, 1):
                hand(u, a, -1, 0, 1, 5, upper)
                hand(u, a, 1, 0, -1, 5, lower)
            blocks(u, 4, 2)
            hand(u, 2, -1, 0, 1, 5, upper)
            hand(u, 2, 1, 0, -1, 5, lower)
        else:
            blocks(u, 5, 4)

    for d in range(1, nseq):
        cnt(d).start()
    kv_buddy(0).start()
    q_out(1).start()
    kv_out(1).start()
    kv_mate(0).start()
    kv_out(2).start()
    kv_out(3).start()
    own_w = pltpu.make_async_copy(
        w_hbm.at[:, :, window(tp)],
        wbuf.at[:, pl.ds(tp * HD, HD), :], w_loc)

    loads[2].wait()
    loads[3].wait()
    for i in range(2):
        cut = lanes(head_of(0) if i == 0 else heads - 1)
        kk = tk_ref[:, cut].astype(F32)
        vv = tv_ref[:, cut].astype(F32)
        tkv[i, 0] = jnp.where(trow_id < plen, kk, kk[0:1, :]).astype(BF16)
        tkv[i, 1] = jnp.where(trow_id < plen, vv, 0.0).astype(BF16)
    tvalid[...] = jnp.where(trow_id < plen, 1.0, 0.0).astype(BF16)
    cbuf[me] = jnp.broadcast_to(count.astype(F32), cbuf.shape[1:])

    def mark(buf, sl, src):
        c = cbuf[src][0:1, :]
        buf[sl * rows:(sl + 1) * rows, :] = jnp.where(row_id.astype(F32) < c, 1.0, 0.0).astype(BF16)

    def mark_home(u):
        for i, zz in enumerate((owner(u), owner(u), other_owner(u), other_owner(u))):
            mark(valid_h, 4 * u + i, zz * 2 + (core if i % 2 == 0 else 1 - core))

    def mark_ring(sl):
        if sl < 2:
            zz, other = z, sl
        elif sl >= 14:
            zz, other = lax.rem(z + 4, nz), sl - 14
        else:
            s, r = 1 + (sl - 2) // 4, (sl - 2) % 4
            zz = lax.rem(z + nz - s, nz) if r < 2 else lax.rem(z + s, nz)
            other = r % 2
        mark(valid_r, sl, zz * 2 + (core if other == 0 else 1 - core))

    def spread(x, n):
        full, rest = divmod(n, HD)
        parts = [x] * full + ([x[:, :rest]] if rest else [])
        return parts[0] if len(parts) == 1 else jnp.concatenate(parts, axis=1)

    def attend(u, tiles, first=False):
        q = qring[...] if isinstance(u, int) and u == units else qhome[u]
        held = None
        for tile in [*tiles, None]:
            fresh = None
            if tile is not None:
                k, v, ok = tile
                fresh = (v, ok, lax.dot_general(q, k, (((1,), (1,)), ((), ())), preferred_element_type=F32))
            if held is not None:
                v, ok, s = held
                n = s.shape[1]
                mb = jnp.max(s, axis=1, keepdims=True) * scale
                if first:
                    m_new = jnp.broadcast_to(mb, (rows, HD))
                else:
                    m_old = m_ref[u]
                    m_new = jnp.maximum(m_old, mb)
                p = jnp.exp2(s * scale - spread(m_new, n)).astype(BF16)
                pv = lax.dot_general(p, jnp.concatenate([v, ok], axis=1), (((1,), (0,)), ((), ())),
                                     preferred_element_type=F32)
                if first:
                    acc[u] = pv
                else:
                    shrink = jnp.exp2(m_old - m_new)
                    acc[u] = acc[u] * jnp.concatenate([shrink, shrink], axis=1) + pv
                m_ref[u] = m_new
            held = fresh

    def text(u):
        i = 1 if isinstance(u, int) and u == units else 0
        attend(u, [(tkv[i, 0], tkv[i, 1], tvalid[...])], first=True)

    def cuts(kv, ok, start, n):
        done, out = 0, []
        while done < n * rows:
            size = min(1024 if n > 2 else 512, n * rows - done)
            r = pl.ds(pl.multiple_of(start * rows + done, 32), size)
            out.append((kv[0, r, :], kv[1, r, :], ok[r, :]))
            done += size
        return out

    def group(u, g):
        attend(u, cuts(kvh, valid_h, 4 * g, 4))

    def stretch(sl, n):
        attend(units, cuts(kvr, valid_r, sl, n))

    def finish(u, put):
        for part in range(2):
            r = pl.ds(part * half, half)
            put(r, (acc[u, r, 0:HD] / acc[u, r, HD:2 * HD]).astype(BF16))

    def to_obuf(u):
        def put(r, x):
            obuf[u, spot, r, :] = x
        finish(u, put)

    def to_owner(u):
        def put(r, x):
            oback[u - 1, r, :] = x
        finish(u, put)
        o_back(u).start()

    def project(u):
        h = head_of(u) if u < units else heads - 1
        with scope(f"proj{u}"):
            for c in range(2):
                lhs = jnp.concatenate([obuf[u, c * ntp + j] for j in range(ntp)], axis=1)
                oacc[c] += jnp.dot(lhs, wbuf[h], preferred_element_type=F32)

    def arrive(u):
        with scope(f"kv{u}"):
            kv_out(u).wait_recv()
            kv_buddy(u).start()
            kv_mate(u).start()

    def arrive_buddy(u):
        with scope(f"kb{u}"):
            kv_buddy(u).wait_recv()
            kv_buddy_mate(u).start()

    def ready(u):
        with scope(f"kd{u}"):
            kv_mate(u).wait_recv()
            kv_buddy_mate(u).wait_recv()

    oacc[...] = jnp.zeros_like(oacc)
    text(0)
    with scope("counts"):
        bytes_of(cbuf.at[0:nseq - 1, 0:1, :], cnt_recv)
    mark_home(0)
    arrive_buddy(0)

    def hop(s, which):
        with scope(f"{'kv'[which]}r{s}"):
            pass_on(which, s)
            pass_on(2 + which, s)

    def wait_q(u):
        with scope(f"q{u}"):
            q_out(u).wait_recv()

    def weights_out():
        own_w.start()
        for d in range(1, ntp):
            wcopy(d).start()

    def weights_in():
        with scope("ww"):
            bytes_of(wbuf.at[:, 0:(ntp - 1) * 64, :], w_recv)
            for d in range(1, ntp):
                wmate(d).start()

    def launch():
        ring(0, 1).start()
        ring(2, 1).start()
        ring(1, 1).start()
        ring(3, 1).start()
        d2d(0, 0).start()
        d2d(1, 0).start()

    def x4():
        with scope("x4"):
            pass_on(0, 4)
            pass_on(3, 4)

    order = [(0, 0), (1, 0), (0, 1), (1, 1), (0, 2), (1, 2), (0, 3), (1, 3),
             (2, 0), (2, 1), (2, 2), (2, 3), (3, 0), (3, 1), (3, 2), (3, 3)]
    ahead = {
        0: [lambda: arrive(1), lambda: ready(0)],
        1: [weights_out, lambda: wait_q(1), lambda: mark_home(1)],
        2: [lambda: arrive(2), lambda: arrive_buddy(1), lambda: arrive(3), lambda: ready(1)],
        3: [lambda: mark_home(2)],
        4: [lambda: arrive_buddy(2), q_out(2).start, lambda: ready(2)],
        5: [lambda: mark_home(3)],
        6: [lambda: arrive_buddy(3), q_out(3).start, lambda: ready(3)],
        7: [lambda: to_obuf(0), lambda: relay(0, 0)],
        8: [lambda: to_owner(1), launch, lambda: wait_q(2)],
        9: [lambda: relay(0, 1)],
        10: [lambda: relay(1, 0), weights_in],
        11: [lambda: relay(0, 2), lambda: hop(1, 0)],
        12: [lambda: to_owner(2), lambda: wait_q(3)],
        13: [lambda: relay(0, 3), lambda: hop(1, 1)],
        14: [lambda: relay(1, 1)],
        15: [lambda: hop(2, 0)],
    }

    def work(k, _):
        for j, steps in ahead.items():
            @pl.when(k == j)
            def _(steps=steps):
                for step in steps:
                    step()
        u, g = jnp.int32(0), jnp.int32(0)
        for j, (a, b) in enumerate(order):
            u = jnp.where(k == j, a, u)
            g = jnp.where(k == j, b, g)

        @pl.when((g == 0) & (k > 0))
        def _():
            text(u)
        group(u, g)
        return 0

    lax.fori_loop(0, len(order), work, 0)
    to_owner(3)
    relay(2, 0)
    relay(1, 2)
    hop(2, 1)
    text(units)
    hop(3, 0)
    d2d(0, 0).wait_recv()
    d2d(1, 0).wait_recv()
    for sl in range(2):
        mark_ring(sl)
    stretch(0, 2)
    relay(1, 3)
    relay(2, 1)
    hop(3, 1)

    def far(s, _):
        @pl.when(s == 0)
        def _():
            d_in(1)
            for sl in range(2, 6):
                mark_ring(sl)

        @pl.when(s == 1)
        def _():
            relay(3, 0)
            d_in(2)
            for sl in range(6, 10):
                mark_ring(sl)

        @pl.when(s == 2)
        def _():
            x4()
            relay(2, 2)
            d_in(3)
            for sl in range(10, 16):
                mark_ring(sl)
        stretch(2 + 4 * s, 4)
        return 0

    lax.fori_loop(0, 3, far, 0)
    with scope("ww2"):
        bytes_of(wbuf.at[:, 0:(ntp - 1) * 64, :], wd_recv)
        own_w.wait()
    d_in(4)
    stretch(14, 2)
    to_obuf(units)
    relay(units, 0)
    relay(0, 4)
    project(0)
    relay(3, 1)
    relay(2, 3)
    relay(1, 4)
    project(1)
    relay(3, 2)
    relay(units, 1)
    relay(3, 3)
    relay(2, 4)
    project(2)
    relay(units, 2)
    relay(units, 3)
    relay(3, 4)
    project(3)
    relay(units, 4)
    project(units)

    cond = oacc[0].astype(BF16).astype(F32)
    uncond = oacc[1].astype(BF16).astype(F32)
    guided = uncond + GUIDANCE * (cond - uncond)
    live = lax.broadcasted_iota(jnp.int32, (rows, wide), 0) < count
    gl = jnp.where(live, guided, 0.0)
    cl = jnp.where(live, cond, 0.0)
    sums = [jnp.sum(t, axis=0, keepdims=True) for t in (gl, gl * gl, cl, cl * cl)]
    tiles = wide // HD
    lines = [t[:, i * HD:(i + 1) * HD] for t in sums for i in range(tiles)]
    stat[...] = jnp.concatenate(lines + [jnp.zeros((16 - 4 * tiles, HD), F32)], axis=0)
    statbuf[me] = stat[...]

    def st(d):
        return remote(stat, statbuf.at[me], st_send, st_recv, seq=lax.rem(me + d, nseq))

    for d in range(1, nseq):
        st(d).start()
    with scope("stats"):
        bytes_of(statbuf.at[0:nseq - 1], st_recv)
    total = statbuf[0]
    number = cbuf[0][0:1, :]
    for i in range(1, nseq):
        total = total + statbuf[i]
        number = number + cbuf[i][0:1, :]
    number = spread(number, wide)
    g_sum, g_square, c_sum, c_square = (
        jnp.concatenate([total[j * tiles + i:j * tiles + i + 1] for i in range(tiles)], axis=1)
        for j in range(4))
    g_mean = g_sum / number
    g_var = g_square / number - g_mean * g_mean
    c_mean = c_sum / number
    c_var = c_square / number - c_mean * c_mean
    factor = RESCALE * jnp.sqrt((c_var + 1.0) / (g_var + 1.0)) + (1.0 - RESCALE)
    vel = g_mean + (guided - g_mean) * factor
    keep = wide - 64
    out_ref[...] = jnp.where(cfg == 0, vel[:, :keep], vel[:, 64:]).astype(BF16)

    with scope("drain"):
        bytes_of(qhome.at[0:3], q_send)
        bytes_of(kvh.at[:, 0:7 * rows, :], kv_send)
        bytes_of(kvh.at[:, 0:8 * rows, :], kd_send)
        bytes_of(kvr.at[:, 0:7 * rows, :], ring_send)
        bytes_of(kvr.at[:, 0:8 * rows, :], d2d_send)
        bytes_of(oback, back_send)
        bytes_of(obuf.at[:, 0:nplane - 1], o_send)
        bytes_of(cbuf.at[0:nseq - 1, 0:1, :], cnt_send)
        bytes_of(statbuf.at[0:nseq - 1], st_send)
        bytes_of(wbuf.at[:, 0:(ntp - 1) * 64, :], w_send)
        bytes_of(wbuf.at[:, 0:(ntp - 1) * 64, :], wd_send)


def body(queries, keys, values, text_keys, text_values, prompt_lengths, frame_counts, out_weight):
    rows, width = queries.shape[1:]
    trows = text_keys.shape[1]
    heads = width // HD
    nseq, ntp = lax.axis_size("seq"), lax.axis_size("tp")
    model = out_weight.shape[1]
    cols = model // ntp
    keep = cols // 2
    wide = keep + 64
    vm = pl.BlockSpec(memory_space=pltpu.VMEM)
    sm = pl.BlockSpec(memory_space=pltpu.SMEM)
    hbm = pl.BlockSpec(memory_space=pl.ANY)
    dma = pltpu.SemaphoreType.DMA
    return pl.pallas_call(
        functools.partial(kernel, (heads, rows, trows, nseq, ntp, cols)),
        out_shape=jax.ShapeDtypeStruct((rows, keep), BF16),
        in_specs=[sm, sm, hbm, hbm, hbm, hbm, hbm, hbm],
        out_specs=vm,
        scratch_shapes=[
            pltpu.VMEM((rows, width), BF16),
            pltpu.VMEM((rows, width), BF16),
            pltpu.VMEM((trows, width), BF16),
            pltpu.VMEM((trows, width), BF16),
            pltpu.VMEM((8, HD), F32),
            pltpu.VMEM((3, rows, HD), BF16),
            pltpu.VMEM((3, 2, rows, HD), BF16),
            pltpu.VMEM((4, rows, HD), BF16),
            pltpu.VMEM((rows, HD), BF16),
            pltpu.VMEM((2, nseq * rows, HD), BF16),
            pltpu.VMEM((2, nseq * rows, HD), BF16),
            pltpu.VMEM((nseq * rows, HD), BF16),
            pltpu.VMEM((nseq * rows, HD), BF16),
            pltpu.VMEM((2, 2, trows, HD), BF16),
            pltpu.VMEM((trows, HD), BF16),
            pltpu.VMEM((nseq, 8, HD), F32),
            pltpu.VMEM((5, rows, HD), F32),
            pltpu.VMEM((5, rows, 2 * HD), F32),
            pltpu.VMEM((3, rows, HD), BF16),
            pltpu.VMEM((heads, 2 * ntp, rows, HD), BF16),
            pltpu.VMEM((heads, ntp * HD, wide), BF16),
            pltpu.VMEM((2, rows, wide), F32),
            pltpu.VMEM((16, HD), F32),
            pltpu.VMEM((nseq, 16, HD), F32),
            dma, dma((3,)), dma, dma((3,)), dma((4,)), dma, dma((4,)), dma((4,)),
            dma, dma((4, 4)), dma, dma((2, 8)), dma, dma, dma, dma((3,)),
            dma, dma((heads, 6)), dma, dma, dma, dma, dma, dma((9,)),
            dma, dma,
        ],
        compiler_params=pltpu.CompilerParams(
            collective_id=0, has_side_effects=True, vmem_limit_bytes=60 * 1024 * 1024
        ),
    )(
        prompt_lengths, frame_counts, queries[0], keys[0], values[0],
        text_keys[0], text_values[0], out_weight.reshape(heads, HD, model),
    )


def solution(mesh):
    placed = (
        P("cfg", "seq", "tp"),
        P("cfg", "seq", "tp"),
        P("cfg", "seq", "tp"),
        P("cfg", None, "tp"),
        P("cfg", None, "tp"),
        P("cfg"),
        P("seq"),
        P("tp", None),
    )
    return jax.shard_map(
        body, mesh=mesh, in_specs=placed, out_specs=P("seq", ("tp", "cfg")), check_vma=False
    )
```

```python
import functools

import jax
import jax.numpy as jnp
from jax import lax
from jax.experimental import pallas as pl
from jax.experimental.pallas import tpu as pltpu
from jax.sharding import PartitionSpec as P

MESH = pl.DeviceIdType.MESH
HD = 128
GUIDANCE = 5.0
RESCALE = 0.7
NEGATIVE = -1e30
LOG2E = 1.4426950408889634
F32 = jnp.float32
BF16 = jnp.bfloat16


def kernel(
    dims,
    plen_ref, count_ref, q_hbm, k_hbm, v_hbm, tk_hbm, tv_hbm, w_hbm,
    out_ref,
    k_ref, v_ref, tk_ref, tv_ref, cnt_in, qout, kvout, qhome, qring,
    kvh, kvr, valid_h, valid_r, tkv, tvalid, cbuf, m_ref, acc, oback, obuf, wbuf,
    oacc, stat, statbuf,
    q_send, q_recv, kv_send, kv_recv, kb_recv, kd_send, kd_recv, kbd_recv,
    ring_send, ring_recv, d2d_send, d2d_recv, cnt_send, cnt_recv, back_send, back_recv,
    o_send, o_recv, w_send, w_recv, wd_send, wd_recv, w_loc, in_sem,
    st_send, st_recv,
):
    heads, rows, trows, nseq, ntp, cols = dims
    nz = nseq // 2
    units = 4
    half = rows // 2
    wide = out_ref.shape[1] + 64
    scale = HD ** (-0.5) * LOG2E
    me = lax.axis_index("seq")
    tp = lax.axis_index("tp")
    cfg = lax.axis_index("cfg")
    z = me // 2
    core = lax.rem(me, 2)
    odd = lax.rem(z, 2)
    up = lax.rem(z + 1, nz) * 2 + core
    down = lax.rem(z + nz - 1, nz) * 2 + core
    mate = z * 2 + (1 - core)
    buddy = (z + 1 - 2 * odd) * 2 + core
    nplane = 2 * ntp
    spot = cfg * ntp + tp
    side = 4
    step_a = jnp.where(core == 0, 1, side)
    step_b = jnp.where(core == 0, side, 1)
    pa = lax.rem(spot // step_a, side)
    pb = lax.rem(spot // step_b, side)

    def place(da, db):
        return lax.rem(pa + da + side, side) * step_a + lax.rem(pb + db + side, side) * step_b

    def target(u):
        flip = lax.rem(odd + u, 2)
        return lax.rem(z + nz + u * (1 - 2 * flip), nz)

    def owner(u):
        return lax.rem(z + nz + u * (2 * odd - 1), nz)

    def other_owner(u):
        return lax.rem(z + nz - (1 + u) * (2 * odd - 1), nz)

    def head_of(u):
        return target(u) // 2 if u else z // 2

    def lanes(h):
        return pl.ds(pl.multiple_of(h * HD, HD), HD)

    count = count_ref[0]
    plen = plen_ref[0]
    scope = jax.named_scope

    def remote(src, dst, ss, rs, **to):
        return pltpu.make_async_remote_copy(
            src_ref=src, dst_ref=dst, send_sem=ss, recv_sem=rs,
            device_id=to, device_id_type=MESH,
        )

    def bytes_of(ref, sem):
        pltpu.make_async_copy(ref, ref, sem).wait()

    pairs = [(k_hbm, k_ref), (v_hbm, v_ref), (tk_hbm, tk_ref), (tv_hbm, tv_ref),
             (q_hbm.at[:, lanes(head_of(0))], qhome.at[0]),
             (q_hbm.at[:, lanes(heads - 1)], qring)]
    pairs += [(q_hbm.at[:, lanes(head_of(u))], qout.at[u - 1]) for u in range(1, units)]
    loads = [pltpu.make_async_copy(a, b, in_sem.at[i]) for i, (a, b) in enumerate(pairs)]
    for copy in loads:
        copy.start()
    barrier = pltpu.get_barrier_semaphore()
    for d in range(1, nseq):
        pl.semaphore_signal(barrier, inc=1, device_id={"seq": lax.rem(me + d, nseq)}, device_id_type=MESH)
    for d in range(1, nplane):
        peer = lax.rem(spot + d, nplane)
        pl.semaphore_signal(barrier, inc=1, device_id={"cfg": peer // ntp, "tp": lax.rem(peer, ntp)},
                            device_id_type=MESH)
    cnt_in[...] = jnp.broadcast_to(count.astype(F32), cnt_in.shape)
    loads[0].wait()
    loads[1].wait()

    row_id = lax.broadcasted_iota(jnp.int32, (rows, HD), 0)
    trow_id = lax.broadcasted_iota(jnp.int32, (trows, HD), 0)
    def prepare(u):
        cut = lanes(head_of(u) if u < units else heads - 1)
        kk = k_ref[:, cut].astype(F32)
        vv = v_ref[:, cut].astype(F32)
        kk = jnp.where(row_id < count, kk, kk[0:1, :]).astype(BF16)
        vv = jnp.where(row_id < count, vv, 0.0).astype(BF16)
        if u == 0:
            kvh[0, 0:rows, :] = kk
            kvh[1, 0:rows, :] = vv
        elif u < units:
            kvout[u - 1, 0] = kk
            kvout[u - 1, 1] = vv
        else:
            kvr[0, 0:rows, :] = kk
            kvr[1, 0:rows, :] = vv

    for u in range(2):
        prepare(u)
    for copy in loads[4:]:
        copy.wait()

    with scope("entry"):
        pl.semaphore_wait(barrier, nseq - 1 + nplane - 1)

    def hslot(i):
        return kvh.at[:, pl.ds(i * rows, rows), :]

    def q_out(u):
        return remote(qout.at[u - 1], qhome.at[u], q_send, q_recv.at[u - 1], seq=target(u) * 2 + core)

    def kv_out(u):
        return remote(kvout.at[u - 1], hslot(4 * u), kv_send, kv_recv.at[u - 1], seq=target(u) * 2 + core)

    def kv_buddy(u):
        return remote(hslot(4 * u), hslot(4 * u + 2), kv_send, kb_recv.at[u], seq=buddy)

    def kv_mate(u):
        return remote(hslot(4 * u), hslot(4 * u + 1), kd_send, kd_recv.at[u], seq=mate)

    def kv_buddy_mate(u):
        return remote(hslot(4 * u + 2), hslot(4 * u + 3), kd_send, kbd_recv.at[u], seq=mate)

    def o_back(u):
        return remote(oback.at[u - 1], obuf.at[u, spot], back_send, back_recv.at[u - 1], seq=owner(u) * 2 + core)

    def slot(kind, s):
        if s == 4:
            return 14
        return 2 + 4 * (s - 1) + (0 if kind < 2 else 2)

    def at(kind, sl):
        return kvr.at[kind % 2, pl.ds(sl * rows, rows), :]

    def last(kind):
        return 4 if kind in (0, 3) else 3

    def ring(kind, s):
        src = at(kind, 0 if s == 1 else slot(kind, s - 1))
        return remote(src, at(kind, slot(kind, s)), ring_send,
                      ring_recv.at[kind, s - 1], seq=(up if kind < 2 else down))

    def d2d(kind, s):
        sl = 0 if s == 0 else slot(kind, s)
        i = {0: 0, 4: 7}.get(s, s if kind < 2 else 3 + s)
        return remote(at(kind, sl), at(kind, sl + 1), d2d_send,
                      d2d_recv.at[kind % 2, i], seq=mate)

    def pass_on(kind, s):
        if s > last(kind):
            return
        ring(kind, s).wait_recv()
        if s < last(kind):
            ring(kind, s + 1).start()
        d2d(kind, s).start()

    def d_in(s):
        for kind in range(4):
            if s <= last(kind) and (s < 4 or kind in (0, 3)):
                d2d(kind, s).wait_recv()

    def cnt(d):
        peer = lax.rem(me + d, nseq)
        return remote(cnt_in.at[0:1, :], cbuf.at[me, 0:1, :], cnt_send, cnt_recv, seq=peer)

    def window(who):
        return pl.ds(pl.multiple_of(who * cols + cfg * (cols - wide), HD), wide)

    def wcopy(d):
        peer = lax.rem(tp + d, ntp)
        return remote(
            w_hbm.at[:, pl.ds(core * 64, 64), window(peer)],
            wbuf.at[:, pl.ds(tp * HD + core * 64, 64), :],
            w_send, w_recv, tp=peer)

    def wmate(d):
        src = lax.rem(tp + ntp - d, ntp)
        part = wbuf.at[:, pl.ds(src * HD + core * 64, 64), :]
        return remote(part, part, wd_send, wd_recv, seq=mate)

    upper, lower = slice(0, half), slice(half, rows)

    def hand(u, da, db, ta, tb, stage, r=None):
        part = obuf.at[u, place(da, db)]
        if r is not None:
            part = obuf.at[u, place(da, db), r, :]
        peer = place(ta, tb)
        remote(part, part, o_send, o_recv.at[u, stage],
               cfg=peer // ntp, tp=lax.rem(peer, ntp)).start()

    def blocks(u, stage, n):
        bytes_of(obuf.at[u, 0:n], o_recv.at[u, stage])

    def relay(u, stage):
        with scope(f"R{u}{stage}"):
            relay_step(u, stage)

    def relay_step(u, stage):
        if stage == 0:
            if 0 < u < units:
                o_back(u).wait_recv()
            for d in (1, -1):
                hand(u, 0, 0, d, 0, 0)
            for d in (1, -1):
                hand(u, 0, 0, 0, d, 2)
        elif stage == 1:
            blocks(u, 0, 2)
            hand(u, -1, 0, 1, 0, 1, upper)
            hand(u, 1, 0, -1, 0, 1, lower)
            for a in (-1, 1):
                for d in (1, -1):
                    hand(u, a, 0, 0, d, 3 if a < 0 else 6)
            blocks(u, 2, 2)
            hand(u, 0, -1, 0, 1, 5, upper)
            hand(u, 0, 1, 0, -1, 5, lower)
        elif stage == 2:
            blocks(u, 1, 1)
            for d in (1, -1):
                hand(u, 2, 0, 0, d, 4)
        elif stage == 3:
            for a in (-1, 1):
                blocks(u, 3 if a < 0 else 6, 2)
                hand(u, a, -1, 0, 1, 5, upper)
                hand(u, a, 1, 0, -1, 5, lower)
            blocks(u, 4, 2)
            hand(u, 2, -1, 0, 1, 5, upper)
            hand(u, 2, 1, 0, -1, 5, lower)
        else:
            blocks(u, 5, 4)

    for d in range(1, nseq):
        cnt(d).start()
    kv_buddy(0).start()
    q_out(1).start()
    kv_out(1).start()
    kv_mate(0).start()
    for u in range(2, units):
        prepare(u)
        kv_out(u).start()
    prepare(units)
    own_w = pltpu.make_async_copy(
        w_hbm.at[:, :, window(tp)],
        wbuf.at[:, pl.ds(tp * HD, HD), :], w_loc)

    loads[2].wait()
    loads[3].wait()
    for i in range(2):
        cut = lanes(head_of(0) if i == 0 else heads - 1)
        kk = tk_ref[:, cut].astype(F32)
        vv = tv_ref[:, cut].astype(F32)
        tkv[i, 0] = jnp.where(trow_id < plen, kk, kk[0:1, :]).astype(BF16)
        tkv[i, 1] = jnp.where(trow_id < plen, vv, 0.0).astype(BF16)
    tvalid[...] = jnp.where(trow_id < plen, 1.0, 0.0).astype(BF16)
    cbuf[me] = jnp.broadcast_to(count.astype(F32), cbuf.shape[1:])

    def mark(buf, sl, src):
        c = cbuf[src][0:1, :]
        buf[sl * rows:(sl + 1) * rows, :] = jnp.where(row_id.astype(F32) < c, 1.0, 0.0).astype(BF16)

    def mark_home(u):
        for i, zz in enumerate((owner(u), owner(u), other_owner(u), other_owner(u))):
            mark(valid_h, 4 * u + i, zz * 2 + (core if i % 2 == 0 else 1 - core))

    def mark_ring(sl):
        if sl < 2:
            zz, other = z, sl
        elif sl >= 14:
            zz, other = lax.rem(z + 4, nz), sl - 14
        else:
            s, r = 1 + (sl - 2) // 4, (sl - 2) % 4
            zz = lax.rem(z + nz - s, nz) if r < 2 else lax.rem(z + s, nz)
            other = r % 2
        mark(valid_r, sl, zz * 2 + (core if other == 0 else 1 - core))

    def spread(x, n):
        full, rest = divmod(n, HD)
        parts = [x] * full + ([x[:, :rest]] if rest else [])
        return parts[0] if len(parts) == 1 else jnp.concatenate(parts, axis=1)

    def attend(u, tiles, first=False):
        q = qring[...] if isinstance(u, int) and u == units else qhome[u]
        held = None
        for tile in [*tiles, None]:
            fresh = None
            if tile is not None:
                k, v, ok = tile
                fresh = (v, ok, lax.dot_general(q, k, (((1,), (1,)), ((), ())), preferred_element_type=F32))
            if held is not None:
                v, ok, s = held
                n = s.shape[1]
                mb = jnp.max(s, axis=1, keepdims=True) * scale
                if first:
                    m_new = jnp.broadcast_to(mb, (rows, HD))
                else:
                    m_old = m_ref[u]
                    m_new = jnp.maximum(m_old, mb)
                p = jnp.exp2(s * scale - spread(m_new, n)).astype(BF16)
                pv = lax.dot_general(p, jnp.concatenate([v, ok], axis=1), (((1,), (0,)), ((), ())),
                                     preferred_element_type=F32)
                if first:
                    acc[u] = pv
                else:
                    shrink = jnp.exp2(m_old - m_new)
                    acc[u] = acc[u] * jnp.concatenate([shrink, shrink], axis=1) + pv
                m_ref[u] = m_new
            held = fresh

    def text(u):
        i = 1 if isinstance(u, int) and u == units else 0
        attend(u, [(tkv[i, 0], tkv[i, 1], tvalid[...])], first=True)

    def cuts(kv, ok, start, n):
        done, out = 0, []
        while done < n * rows:
            size = min(1024 if n > 2 else 512, n * rows - done)
            r = pl.ds(pl.multiple_of(start * rows + done, 32), size)
            out.append((kv[0, r, :], kv[1, r, :], ok[r, :]))
            done += size
        return out

    def group(u, g):
        attend(u, cuts(kvh, valid_h, 4 * g, 4))

    def stretch(sl, n):
        attend(units, cuts(kvr, valid_r, sl, n))

    def finish(u, put):
        for part in range(2):
            r = pl.ds(part * half, half)
            put(r, (acc[u, r, 0:HD] / acc[u, r, HD:2 * HD]).astype(BF16))

    def to_obuf(u):
        def put(r, x):
            obuf[u, spot, r, :] = x
        finish(u, put)

    def to_owner(u):
        def put(r, x):
            oback[u - 1, r, :] = x
        finish(u, put)
        o_back(u).start()

    def project(u):
        h = head_of(u) if u < units else heads - 1
        with scope(f"proj{u}"):
            for c in range(2):
                lhs = jnp.concatenate([obuf[u, c * ntp + j] for j in range(ntp)], axis=1)
                oacc[c] += jnp.dot(lhs, wbuf[h], preferred_element_type=F32)

    def arrive(u):
        with scope(f"kv{u}"):
            kv_out(u).wait_recv()
            kv_buddy(u).start()
            kv_mate(u).start()

    def arrive_buddy(u):
        with scope(f"kb{u}"):
            kv_buddy(u).wait_recv()
            kv_buddy_mate(u).start()

    def ready(u):
        with scope(f"kd{u}"):
            kv_mate(u).wait_recv()
            kv_buddy_mate(u).wait_recv()

    oacc[...] = jnp.zeros_like(oacc)
    text(0)
    with scope("counts"):
        bytes_of(cbuf.at[0:nseq - 1, 0:1, :], cnt_recv)
    mark_home(0)
    arrive_buddy(0)

    def hop(s, which):
        with scope(f"{'kv'[which]}r{s}"):
            pass_on(which, s)
            pass_on(2 + which, s)

    def wait_q(u):
        with scope(f"q{u}"):
            q_out(u).wait_recv()

    def weights_out():
        own_w.start()
        for d in range(1, ntp):
            wcopy(d).start()

    def weights_in():
        with scope("ww"):
            bytes_of(wbuf.at[:, 0:(ntp - 1) * 64, :], w_recv)
            for d in range(1, ntp):
                wmate(d).start()

    def launch():
        ring(0, 1).start()
        ring(2, 1).start()
        ring(1, 1).start()
        ring(3, 1).start()
        d2d(0, 0).start()
        d2d(1, 0).start()

    def x4():
        with scope("x4"):
            pass_on(0, 4)
            pass_on(3, 4)

    order = [(0, 0), (1, 0), (0, 1), (1, 1), (0, 2), (0, 3), (1, 2), (1, 3),
             (2, 0), (2, 1), (2, 2), (2, 3), (3, 0), (3, 1), (3, 2), (3, 3)]
    ahead = {
        0: [lambda: arrive(1), lambda: ready(0)],
        1: [weights_out, lambda: wait_q(1), lambda: mark_home(1)],
        2: [lambda: arrive(2), lambda: arrive_buddy(1), lambda: arrive(3), lambda: ready(1)],
        3: [lambda: mark_home(2), lambda: mark_home(3)],
        4: [lambda: arrive_buddy(2), q_out(2).start, lambda: ready(2)],
        5: [lambda: arrive_buddy(3), q_out(3).start, lambda: ready(3)],
        6: [lambda: to_obuf(0), lambda: relay(0, 0)],
        8: [lambda: to_owner(1), launch, lambda: wait_q(2)],
        9: [lambda: relay(0, 1)],
        10: [lambda: relay(1, 0), weights_in],
        11: [lambda: relay(0, 2), lambda: hop(1, 0)],
        12: [lambda: to_owner(2), lambda: wait_q(3)],
        13: [lambda: relay(0, 3), lambda: relay(1, 1)],
        14: [lambda: hop(1, 1)],
        15: [lambda: relay(1, 2), lambda: hop(2, 0)],
    }

    def work(k, _):
        for j, steps in ahead.items():
            @pl.when(k == j)
            def _(steps=steps):
                for step in steps:
                    step()
        u, g = jnp.int32(0), jnp.int32(0)
        for j, (a, b) in enumerate(order):
            u = jnp.where(k == j, a, u)
            g = jnp.where(k == j, b, g)

        @pl.when((g == 0) & (k > 0))
        def _():
            text(u)
        group(u, g)
        return 0

    lax.fori_loop(0, len(order), work, 0)
    to_owner(3)
    relay(2, 0)
    hop(2, 1)
    text(units)
    relay(1, 3)
    d2d(0, 0).wait_recv()
    d2d(1, 0).wait_recv()
    for sl in range(2):
        mark_ring(sl)
    stretch(0, 2)
    relay(2, 1)
    hop(3, 0)
    relay(3, 0)
    relay(2, 2)
    hop(3, 1)

    def far(s, _):
        @pl.when(s == 0)
        def _():
            d_in(1)
            for sl in range(2, 6):
                mark_ring(sl)

        @pl.when(s == 1)
        def _():
            relay(3, 1)
            d_in(2)
            for sl in range(6, 10):
                mark_ring(sl)

        @pl.when(s == 2)
        def _():
            relay(2, 3)
            d_in(3)
            for sl in range(10, 16):
                mark_ring(sl)
        stretch(2 + 4 * s, 4)
        return 0

    lax.fori_loop(0, 3, far, 0)
    x4()
    with scope("ww2"):
        bytes_of(wbuf.at[:, 0:(ntp - 1) * 64, :], wd_recv)
        own_w.wait()
    d_in(4)
    stretch(14, 2)
    to_obuf(units)
    relay(units, 0)
    relay(0, 4)
    project(0)
    relay(3, 2)
    relay(1, 4)
    project(1)
    relay(units, 1)
    relay(3, 3)
    relay(2, 4)
    project(2)
    relay(units, 2)
    relay(units, 3)
    relay(3, 4)
    project(3)
    relay(units, 4)
    project(units)

    cond = oacc[0].astype(BF16).astype(F32)
    uncond = oacc[1].astype(BF16).astype(F32)
    guided = uncond + GUIDANCE * (cond - uncond)
    live = lax.broadcasted_iota(jnp.int32, (rows, wide), 0) < count
    gl = jnp.where(live, guided, 0.0)
    cl = jnp.where(live, cond, 0.0)
    sums = [jnp.sum(t, axis=0, keepdims=True) for t in (gl, gl * gl, cl, cl * cl)]
    tiles = wide // HD
    lines = [t[:, i * HD:(i + 1) * HD] for t in sums for i in range(tiles)]
    stat[...] = jnp.concatenate(lines + [jnp.zeros((16 - 4 * tiles, HD), F32)], axis=0)
    statbuf[me] = stat[...]

    def st(d):
        return remote(stat, statbuf.at[me], st_send, st_recv, seq=lax.rem(me + d, nseq))

    for d in range(1, nseq):
        st(d).start()
    with scope("stats"):
        bytes_of(statbuf.at[0:nseq - 1], st_recv)
    total = statbuf[0]
    number = cbuf[0][0:1, :]
    for i in range(1, nseq):
        total = total + statbuf[i]
        number = number + cbuf[i][0:1, :]
    number = spread(number, wide)
    g_sum, g_square, c_sum, c_square = (
        jnp.concatenate([total[j * tiles + i:j * tiles + i + 1] for i in range(tiles)], axis=1)
        for j in range(4))
    g_mean = g_sum / number
    g_var = g_square / number - g_mean * g_mean
    c_mean = c_sum / number
    c_var = c_square / number - c_mean * c_mean
    factor = RESCALE * jnp.sqrt((c_var + 1.0) / (g_var + 1.0)) + (1.0 - RESCALE)
    vel = g_mean + (guided - g_mean) * factor
    keep = wide - 64
    out_ref[...] = jnp.where(cfg == 0, vel[:, :keep], vel[:, 64:]).astype(BF16)

    with scope("drain"):
        bytes_of(qhome.at[0:3], q_send)
        bytes_of(kvh.at[:, 0:7 * rows, :], kv_send)
        bytes_of(kvh.at[:, 0:8 * rows, :], kd_send)
        bytes_of(kvr.at[:, 0:7 * rows, :], ring_send)
        bytes_of(kvr.at[:, 0:8 * rows, :], d2d_send)
        bytes_of(oback, back_send)
        bytes_of(obuf.at[:, 0:nplane - 1], o_send)
        bytes_of(cbuf.at[0:nseq - 1, 0:1, :], cnt_send)
        bytes_of(statbuf.at[0:nseq - 1], st_send)
        bytes_of(wbuf.at[:, 0:(ntp - 1) * 64, :], w_send)
        bytes_of(wbuf.at[:, 0:(ntp - 1) * 64, :], wd_send)


def body(queries, keys, values, text_keys, text_values, prompt_lengths, frame_counts, out_weight):
    rows, width = queries.shape[1:]
    trows = text_keys.shape[1]
    heads = width // HD
    nseq, ntp = lax.axis_size("seq"), lax.axis_size("tp")
    model = out_weight.shape[1]
    cols = model // ntp
    keep = cols // 2
    wide = keep + 64
    vm = pl.BlockSpec(memory_space=pltpu.VMEM)
    sm = pl.BlockSpec(memory_space=pltpu.SMEM)
    hbm = pl.BlockSpec(memory_space=pl.ANY)
    dma = pltpu.SemaphoreType.DMA
    return pl.pallas_call(
        functools.partial(kernel, (heads, rows, trows, nseq, ntp, cols)),
        out_shape=jax.ShapeDtypeStruct((rows, keep), BF16),
        in_specs=[sm, sm, hbm, hbm, hbm, hbm, hbm, hbm],
        out_specs=vm,
        scratch_shapes=[
            pltpu.VMEM((rows, width), BF16),
            pltpu.VMEM((rows, width), BF16),
            pltpu.VMEM((trows, width), BF16),
            pltpu.VMEM((trows, width), BF16),
            pltpu.VMEM((8, HD), F32),
            pltpu.VMEM((3, rows, HD), BF16),
            pltpu.VMEM((3, 2, rows, HD), BF16),
            pltpu.VMEM((4, rows, HD), BF16),
            pltpu.VMEM((rows, HD), BF16),
            pltpu.VMEM((2, nseq * rows, HD), BF16),
            pltpu.VMEM((2, nseq * rows, HD), BF16),
            pltpu.VMEM((nseq * rows, HD), BF16),
            pltpu.VMEM((nseq * rows, HD), BF16),
            pltpu.VMEM((2, 2, trows, HD), BF16),
            pltpu.VMEM((trows, HD), BF16),
            pltpu.VMEM((nseq, 8, HD), F32),
            pltpu.VMEM((5, rows, HD), F32),
            pltpu.VMEM((5, rows, 2 * HD), F32),
            pltpu.VMEM((3, rows, HD), BF16),
            pltpu.VMEM((heads, 2 * ntp, rows, HD), BF16),
            pltpu.VMEM((heads, ntp * HD, wide), BF16),
            pltpu.VMEM((2, rows, wide), F32),
            pltpu.VMEM((16, HD), F32),
            pltpu.VMEM((nseq, 16, HD), F32),
            dma, dma((3,)), dma, dma((3,)), dma((4,)), dma, dma((4,)), dma((4,)),
            dma, dma((4, 4)), dma, dma((2, 8)), dma, dma, dma, dma((3,)),
            dma, dma((heads, 7)), dma, dma, dma, dma, dma, dma((9,)),
            dma, dma,
        ],
        compiler_params=pltpu.CompilerParams(
            collective_id=0, has_side_effects=True, vmem_limit_bytes=60 * 1024 * 1024
        ),
    )(
        prompt_lengths, frame_counts, queries[0], keys[0], values[0],
        text_keys[0], text_values[0], out_weight.reshape(heads, HD, model),
    )


def solution(mesh):
    placed = (
        P("cfg", "seq", "tp"),
        P("cfg", "seq", "tp"),
        P("cfg", "seq", "tp"),
        P("cfg", None, "tp"),
        P("cfg", None, "tp"),
        P("cfg"),
        P("seq"),
        P("tp", None),
    )
    return jax.shard_map(
        body, mesh=mesh, in_specs=placed, out_specs=P("seq", ("tp", "cfg")), check_vma=False
    )
```

```python
import functools

import jax
import jax.numpy as jnp
from jax import lax
from jax.experimental import pallas as pl
from jax.experimental.pallas import tpu as pltpu
from jax.sharding import PartitionSpec as P

MESH = pl.DeviceIdType.MESH
HD = 128
GUIDANCE = 5.0
RESCALE = 0.7
NEGATIVE = -1e30
LOG2E = 1.4426950408889634
F32 = jnp.float32
BF16 = jnp.bfloat16


def kernel(
    dims,
    plen_ref, count_ref, q_hbm, k_hbm, v_hbm, tk_hbm, tv_hbm, w_hbm,
    out_ref,
    k_ref, v_ref, tk_ref, tv_ref, cnt_in, qout, kvout, qhome, qring,
    kvh, kvr, valid_h, valid_r, tkv, tvalid, cbuf, m_ref, acc, oback, obuf, wbuf,
    oacc, stat, statbuf,
    q_send, q_recv, kv_send, kv_recv, kb_recv, kd_send, kd_recv, kbd_recv,
    ring_send, ring_recv, d2d_send, d2d_recv, cnt_send, cnt_recv, back_send, back_recv,
    o_send, o_recv, w_send, w_recv, wd_send, wd_recv, w_loc, in_sem,
    st_send, st_recv,
):
    heads, rows, trows, nseq, ntp, cols = dims
    nz = nseq // 2
    units = 4
    half = rows // 2
    wide = out_ref.shape[1] + 64
    scale = HD ** (-0.5) * LOG2E
    me = lax.axis_index("seq")
    tp = lax.axis_index("tp")
    cfg = lax.axis_index("cfg")
    z = me // 2
    core = lax.rem(me, 2)
    odd = lax.rem(z, 2)
    up = lax.rem(z + 1, nz) * 2 + core
    down = lax.rem(z + nz - 1, nz) * 2 + core
    mate = z * 2 + (1 - core)
    buddy = (z + 1 - 2 * odd) * 2 + core
    nplane = 2 * ntp
    spot = cfg * ntp + tp
    side = 4
    step_a = jnp.where(core == 0, 1, side)
    step_b = jnp.where(core == 0, side, 1)
    pa = lax.rem(spot // step_a, side)
    pb = lax.rem(spot // step_b, side)

    def place(da, db):
        return lax.rem(pa + da + side, side) * step_a + lax.rem(pb + db + side, side) * step_b

    def target(u):
        flip = lax.rem(odd + u, 2)
        return lax.rem(z + nz + u * (1 - 2 * flip), nz)

    def owner(u):
        return lax.rem(z + nz + u * (2 * odd - 1), nz)

    def other_owner(u):
        return lax.rem(z + nz - (1 + u) * (2 * odd - 1), nz)

    def head_of(u):
        return target(u) // 2 if u else z // 2

    def lanes(h):
        return pl.ds(pl.multiple_of(h * HD, HD), HD)

    count = count_ref[0]
    plen = plen_ref[0]
    scope = jax.named_scope

    def remote(src, dst, ss, rs, **to):
        return pltpu.make_async_remote_copy(
            src_ref=src, dst_ref=dst, send_sem=ss, recv_sem=rs,
            device_id=to, device_id_type=MESH,
        )

    def bytes_of(ref, sem):
        pltpu.make_async_copy(ref, ref, sem).wait()

    pairs = [(k_hbm, k_ref), (v_hbm, v_ref), (tk_hbm, tk_ref), (tv_hbm, tv_ref),
             (q_hbm.at[:, lanes(head_of(0))], qhome.at[0]),
             (q_hbm.at[:, lanes(heads - 1)], qring)]
    pairs += [(q_hbm.at[:, lanes(head_of(u))], qout.at[u - 1]) for u in range(1, units)]
    loads = [pltpu.make_async_copy(a, b, in_sem.at[i]) for i, (a, b) in enumerate(pairs)]
    for copy in loads:
        copy.start()
    barrier = pltpu.get_barrier_semaphore()
    for d in range(1, nseq):
        pl.semaphore_signal(barrier, inc=1, device_id={"seq": lax.rem(me + d, nseq)}, device_id_type=MESH)
    for d in range(1, nplane):
        peer = lax.rem(spot + d, nplane)
        pl.semaphore_signal(barrier, inc=1, device_id={"cfg": peer // ntp, "tp": lax.rem(peer, ntp)},
                            device_id_type=MESH)
    cnt_in[...] = jnp.broadcast_to(count.astype(F32), cnt_in.shape)
    loads[0].wait()
    loads[1].wait()

    row_id = lax.broadcasted_iota(jnp.int32, (rows, HD), 0)
    trow_id = lax.broadcasted_iota(jnp.int32, (trows, HD), 0)
    def prepare(u):
        cut = lanes(head_of(u) if u < units else heads - 1)
        kk = k_ref[:, cut].astype(F32)
        vv = v_ref[:, cut].astype(F32)
        kk = jnp.where(row_id < count, kk, kk[0:1, :]).astype(BF16)
        vv = jnp.where(row_id < count, vv, 0.0).astype(BF16)
        if u == 0:
            kvh[0, 0:rows, :] = kk
            kvh[1, 0:rows, :] = vv
        elif u < units:
            kvout[u - 1, 0] = kk
            kvout[u - 1, 1] = vv
        else:
            kvr[0, 0:rows, :] = kk
            kvr[1, 0:rows, :] = vv

    for u in range(2):
        prepare(u)
    for copy in loads[4:]:
        copy.wait()

    with scope("entry"):
        pl.semaphore_wait(barrier, nseq - 1 + nplane - 1)

    def hslot(i):
        return kvh.at[:, pl.ds(i * rows, rows), :]

    def q_out(u):
        return remote(qout.at[u - 1], qhome.at[u], q_send, q_recv.at[u - 1], seq=target(u) * 2 + core)

    def kv_out(u):
        return remote(kvout.at[u - 1], hslot(4 * u), kv_send, kv_recv.at[u - 1], seq=target(u) * 2 + core)

    def kv_buddy(u):
        return remote(hslot(4 * u), hslot(4 * u + 2), kv_send, kb_recv.at[u], seq=buddy)

    def kv_mate(u):
        return remote(hslot(4 * u), hslot(4 * u + 1), kd_send, kd_recv.at[u], seq=mate)

    def kv_buddy_mate(u):
        return remote(hslot(4 * u + 2), hslot(4 * u + 3), kd_send, kbd_recv.at[u], seq=mate)

    def o_back(u):
        return remote(oback.at[u - 1], obuf.at[u, spot], back_send, back_recv.at[u - 1], seq=owner(u) * 2 + core)

    def slot(kind, s):
        if s == 4:
            return 14
        return 2 + 4 * (s - 1) + (0 if kind < 2 else 2)

    def at(kind, sl):
        return kvr.at[kind % 2, pl.ds(sl * rows, rows), :]

    def last(kind):
        return 4 if kind in (0, 3) else 3

    def ring(kind, s):
        src = at(kind, 0 if s == 1 else slot(kind, s - 1))
        return remote(src, at(kind, slot(kind, s)), ring_send,
                      ring_recv.at[kind, s - 1], seq=(up if kind < 2 else down))

    def d2d(kind, s):
        sl = 0 if s == 0 else slot(kind, s)
        i = {0: 0, 4: 7}.get(s, s if kind < 2 else 3 + s)
        return remote(at(kind, sl), at(kind, sl + 1), d2d_send,
                      d2d_recv.at[kind % 2, i], seq=mate)

    def pass_on(kind, s):
        if s > last(kind):
            return
        ring(kind, s).wait_recv()
        if s < last(kind):
            ring(kind, s + 1).start()
        d2d(kind, s).start()

    def d_in(s):
        for kind in range(4):
            if s <= last(kind) and (s < 4 or kind in (0, 3)):
                d2d(kind, s).wait_recv()

    def cnt(d):
        peer = lax.rem(me + d, nseq)
        return remote(cnt_in.at[0:1, :], cbuf.at[me, 0:1, :], cnt_send, cnt_recv, seq=peer)

    def window(who):
        return pl.ds(pl.multiple_of(who * cols + cfg * (cols - wide), HD), wide)

    def wcopy(d):
        peer = lax.rem(tp + d, ntp)
        return remote(
            w_hbm.at[:, pl.ds(core * 64, 64), window(peer)],
            wbuf.at[:, pl.ds(tp * HD + core * 64, 64), :],
            w_send, w_recv, tp=peer)

    def wmate(d):
        src = lax.rem(tp + ntp - d, ntp)
        part = wbuf.at[:, pl.ds(src * HD + core * 64, 64), :]
        return remote(part, part, wd_send, wd_recv, seq=mate)

    upper, lower = slice(0, half), slice(half, rows)

    def hand(u, da, db, ta, tb, stage, r=None):
        part = obuf.at[u, place(da, db)]
        if r is not None:
            part = obuf.at[u, place(da, db), r, :]
        peer = place(ta, tb)
        remote(part, part, o_send, o_recv.at[u, stage],
               cfg=peer // ntp, tp=lax.rem(peer, ntp)).start()

    def blocks(u, stage, n):
        bytes_of(obuf.at[u, 0:n], o_recv.at[u, stage])

    def relay(u, stage):
        with scope(f"R{u}{stage}"):
            relay_step(u, stage)

    def relay_step(u, stage):
        if stage == 0:
            if 0 < u < units:
                o_back(u).wait_recv()
            for d in (1, -1):
                hand(u, 0, 0, d, 0, 0)
            for d in (1, -1):
                hand(u, 0, 0, 0, d, 2)
        elif stage == 1:
            blocks(u, 0, 2)
            hand(u, -1, 0, 1, 0, 1, upper)
            hand(u, 1, 0, -1, 0, 1, lower)
            for a in (-1, 1):
                for d in (1, -1):
                    hand(u, a, 0, 0, d, 3 if a < 0 else 6)
            blocks(u, 2, 2)
            hand(u, 0, -1, 0, 1, 5, upper)
            hand(u, 0, 1, 0, -1, 5, lower)
        elif stage == 2:
            blocks(u, 1, 1)
            for d in (1, -1):
                hand(u, 2, 0, 0, d, 4)
        elif stage == 3:
            for a in (-1, 1):
                blocks(u, 3 if a < 0 else 6, 2)
                hand(u, a, -1, 0, 1, 5, upper)
                hand(u, a, 1, 0, -1, 5, lower)
            blocks(u, 4, 2)
            hand(u, 2, -1, 0, 1, 5, upper)
            hand(u, 2, 1, 0, -1, 5, lower)
        else:
            blocks(u, 5, 4)

    for d in range(1, nseq):
        cnt(d).start()
    kv_buddy(0).start()
    q_out(1).start()
    kv_out(1).start()
    kv_mate(0).start()
    for u in range(2, units):
        prepare(u)
        kv_out(u).start()
    prepare(units)
    own_w = pltpu.make_async_copy(
        w_hbm.at[:, :, window(tp)],
        wbuf.at[:, pl.ds(tp * HD, HD), :], w_loc)

    loads[2].wait()
    loads[3].wait()
    for i in range(2):
        cut = lanes(head_of(0) if i == 0 else heads - 1)
        kk = tk_ref[:, cut].astype(F32)
        vv = tv_ref[:, cut].astype(F32)
        tkv[i, 0] = jnp.where(trow_id < plen, kk, kk[0:1, :]).astype(BF16)
        tkv[i, 1] = jnp.where(trow_id < plen, vv, 0.0).astype(BF16)
    tvalid[...] = jnp.where(trow_id < plen, 1.0, 0.0).astype(BF16)
    cbuf[me] = jnp.broadcast_to(count.astype(F32), cbuf.shape[1:])

    def mark(buf, sl, src):
        c = cbuf[src][0:1, :]
        buf[sl * rows:(sl + 1) * rows, :] = jnp.where(row_id.astype(F32) < c, 1.0, 0.0).astype(BF16)

    def mark_home(u):
        for i, zz in enumerate((owner(u), owner(u), other_owner(u), other_owner(u))):
            mark(valid_h, 4 * u + i, zz * 2 + (core if i % 2 == 0 else 1 - core))

    def mark_ring(sl):
        if sl < 2:
            zz, other = z, sl
        elif sl >= 14:
            zz, other = lax.rem(z + 4, nz), sl - 14
        else:
            s, r = 1 + (sl - 2) // 4, (sl - 2) % 4
            zz = lax.rem(z + nz - s, nz) if r < 2 else lax.rem(z + s, nz)
            other = r % 2
        mark(valid_r, sl, zz * 2 + (core if other == 0 else 1 - core))

    def spread(x, n):
        full, rest = divmod(n, HD)
        parts = [x] * full + ([x[:, :rest]] if rest else [])
        return parts[0] if len(parts) == 1 else jnp.concatenate(parts, axis=1)

    def attend(u, tiles, first=False):
        q = qring[...] if isinstance(u, int) and u == units else qhome[u]
        held = None
        for tile in [*tiles, None]:
            fresh = None
            if tile is not None:
                k, v, ok = tile
                fresh = (v, ok, lax.dot_general(q, k, (((1,), (1,)), ((), ())), preferred_element_type=F32))
            if held is not None:
                v, ok, s = held
                n = s.shape[1]
                mb = jnp.max(s, axis=1, keepdims=True) * scale
                if first:
                    m_new = jnp.broadcast_to(mb, (rows, HD))
                else:
                    m_old = m_ref[u]
                    m_new = jnp.maximum(m_old, mb)
                p = jnp.exp2(s * scale - spread(m_new, n)).astype(BF16)
                pv = lax.dot_general(p, jnp.concatenate([v, ok], axis=1), (((1,), (0,)), ((), ())),
                                     preferred_element_type=F32)
                if first:
                    acc[u] = pv
                else:
                    shrink = jnp.exp2(m_old - m_new)
                    acc[u] = acc[u] * jnp.concatenate([shrink, shrink], axis=1) + pv
                m_ref[u] = m_new
            held = fresh

    def text(u):
        i = 1 if isinstance(u, int) and u == units else 0
        attend(u, [(tkv[i, 0], tkv[i, 1], tvalid[...])], first=True)

    def cuts(kv, ok, start, n):
        done, out = 0, []
        while done < n * rows:
            size = min(1024 if n > 2 else 512, n * rows - done)
            r = pl.ds(pl.multiple_of(start * rows + done, 32), size)
            out.append((kv[0, r, :], kv[1, r, :], ok[r, :]))
            done += size
        return out

    def group(u, g):
        attend(u, cuts(kvh, valid_h, 4 * g, 4))

    def stretch(sl, n):
        attend(units, cuts(kvr, valid_r, sl, n))

    def finish(u, put):
        for part in range(2):
            r = pl.ds(part * half, half)
            put(r, (acc[u, r, 0:HD] / acc[u, r, HD:2 * HD]).astype(BF16))

    def to_obuf(u):
        def put(r, x):
            obuf[u, spot, r, :] = x
        finish(u, put)

    def to_owner(u):
        def put(r, x):
            oback[u - 1, r, :] = x
        finish(u, put)
        o_back(u).start()

    def project(u):
        h = head_of(u) if u < units else heads - 1
        with scope(f"proj{u}"):
            for c in range(2):
                lhs = jnp.concatenate([obuf[u, c * ntp + j] for j in range(ntp)], axis=1)
                oacc[c] += jnp.dot(lhs, wbuf[h], preferred_element_type=F32)

    def arrive(u):
        with scope(f"kv{u}"):
            kv_out(u).wait_recv()
            kv_buddy(u).start()
            kv_mate(u).start()

    def arrive_buddy(u):
        with scope(f"kb{u}"):
            kv_buddy(u).wait_recv()
            kv_buddy_mate(u).start()

    def ready(u):
        with scope(f"kd{u}"):
            kv_mate(u).wait_recv()
            kv_buddy_mate(u).wait_recv()

    oacc[...] = jnp.zeros_like(oacc)
    text(0)
    with scope("counts"):
        bytes_of(cbuf.at[0:nseq - 1, 0:1, :], cnt_recv)
    mark_home(0)
    arrive_buddy(0)

    def hop(s, which):
        with scope(f"{'kv'[which]}r{s}"):
            pass_on(which, s)
            pass_on(2 + which, s)

    def wait_q(u):
        with scope(f"q{u}"):
            q_out(u).wait_recv()

    def weights_out():
        own_w.start()
        for d in range(1, ntp):
            wcopy(d).start()

    def weights_in():
        with scope("ww"):
            bytes_of(wbuf.at[:, 0:(ntp - 1) * 64, :], w_recv)
            for d in range(1, ntp):
                wmate(d).start()

    def launch():
        ring(0, 1).start()
        ring(2, 1).start()
        ring(1, 1).start()
        ring(3, 1).start()
        d2d(0, 0).start()
        d2d(1, 0).start()

    def mark_all_ring():
        for sl in range(nseq):
            mark_ring(sl)

    def x4():
        with scope("x4"):
            pass_on(0, 4)
            pass_on(3, 4)

    order = [(0, 0), (1, 0), (0, 1), (1, 1), (0, 2), (1, 2), (0, 3), (1, 3),
             (2, 0), (2, 1), (2, 2), (2, 3), (3, 0), (3, 1), (3, 2), (3, 3)]
    ahead = {
        0: [lambda: arrive(1), lambda: ready(0)],
        1: [weights_out, lambda: wait_q(1), lambda: mark_home(1)],
        2: [lambda: arrive(2), mark_all_ring, lambda: arrive_buddy(1), lambda: arrive(3), lambda: ready(1)],
        3: [lambda: mark_home(2), lambda: mark_home(3)],
        4: [lambda: arrive_buddy(2), q_out(2).start, lambda: ready(2)],
        5: [lambda: arrive_buddy(3), q_out(3).start],
        6: [lambda: ready(3)],
        7: [lambda: to_obuf(0), lambda: relay(0, 0)],
        8: [lambda: to_owner(1), launch, lambda: wait_q(2)],
        9: [lambda: relay(0, 1)],
        10: [lambda: relay(1, 0), weights_in],
        11: [lambda: relay(0, 2), lambda: hop(1, 0)],
        12: [lambda: to_owner(2), lambda: wait_q(3)],
        13: [lambda: relay(0, 3), lambda: relay(1, 1)],
        14: [lambda: hop(1, 1)],
        15: [lambda: relay(1, 2), lambda: hop(2, 0)],
    }

    def work(k, _):
        for j, steps in ahead.items():
            @pl.when(k == j)
            def _(steps=steps):
                for step in steps:
                    step()
        u, g = jnp.int32(0), jnp.int32(0)
        for j, (a, b) in enumerate(order):
            u = jnp.where(k == j, a, u)
            g = jnp.where(k == j, b, g)

        @pl.when((g == 0) & (k > 0))
        def _():
            text(u)
        group(u, g)
        return 0

    lax.fori_loop(0, len(order), work, 0)
    to_owner(3)
    relay(2, 0)
    hop(2, 1)
    text(units)
    relay(1, 3)
    d2d(0, 0).wait_recv()
    d2d(1, 0).wait_recv()
    stretch(0, 2)
    relay(2, 1)
    hop(3, 0)
    relay(3, 0)
    relay(2, 2)
    hop(3, 1)

    def far(s, _):
        @pl.when(s == 0)
        def _():
            d_in(1)

        @pl.when(s == 1)
        def _():
            relay(3, 1)
            d_in(2)

        @pl.when(s == 2)
        def _():
            relay(2, 3)
            d_in(3)
        stretch(2 + 4 * s, 4)
        return 0

    lax.fori_loop(0, 3, far, 0)
    x4()
    with scope("ww2"):
        bytes_of(wbuf.at[:, 0:(ntp - 1) * 64, :], wd_recv)
        own_w.wait()
    d_in(4)
    stretch(14, 2)
    to_obuf(units)
    relay(units, 0)
    relay(0, 4)
    project(0)
    relay(3, 2)
    relay(1, 4)
    project(1)
    relay(units, 1)
    relay(3, 3)
    relay(2, 4)
    project(2)
    relay(units, 2)
    relay(units, 3)
    relay(3, 4)
    project(3)
    relay(units, 4)
    project(units)

    cond = oacc[0].astype(BF16).astype(F32)
    uncond = oacc[1].astype(BF16).astype(F32)
    guided = uncond + GUIDANCE * (cond - uncond)
    live = lax.broadcasted_iota(jnp.int32, (rows, wide), 0) < count
    gl = jnp.where(live, guided, 0.0)
    cl = jnp.where(live, cond, 0.0)
    sums = [jnp.sum(t, axis=0, keepdims=True) for t in (gl, gl * gl, cl, cl * cl)]
    tiles = wide // HD
    lines = [t[:, i * HD:(i + 1) * HD] for t in sums for i in range(tiles)]
    stat[...] = jnp.concatenate(lines + [jnp.zeros((16 - 4 * tiles, HD), F32)], axis=0)
    statbuf[me] = stat[...]

    lead = 4 * tiles

    def st(d):
        return remote(stat.at[0:lead, :], statbuf.at[me, 0:lead, :], st_send, st_recv, seq=lax.rem(me + d, nseq))

    for d in range(1, nseq):
        st(d).start()
    with scope("stats"):
        bytes_of(statbuf.at[0:nseq - 1, 0:lead, :], st_recv)
    total = statbuf[0, 0:lead, :]
    number = cbuf[0][0:1, :]
    for i in range(1, nseq):
        total = total + statbuf[i, 0:lead, :]
        number = number + cbuf[i][0:1, :]
    number = spread(number, wide)
    g_sum, g_square, c_sum, c_square = (
        jnp.concatenate([total[j * tiles + i:j * tiles + i + 1] for i in range(tiles)], axis=1)
        for j in range(4))
    g_mean = g_sum / number
    g_var = g_square / number - g_mean * g_mean
    c_mean = c_sum / number
    c_var = c_square / number - c_mean * c_mean
    factor = RESCALE * jnp.sqrt((c_var + 1.0) / (g_var + 1.0)) + (1.0 - RESCALE)
    vel = g_mean + (guided - g_mean) * factor
    keep = wide - 64
    out_ref[...] = jnp.where(cfg == 0, vel[:, :keep], vel[:, 64:]).astype(BF16)

    with scope("drain"):
        bytes_of(qhome.at[0:3], q_send)
        bytes_of(kvh.at[:, 0:7 * rows, :], kv_send)
        bytes_of(kvh.at[:, 0:8 * rows, :], kd_send)
        bytes_of(kvr.at[:, 0:7 * rows, :], ring_send)
        bytes_of(kvr.at[:, 0:8 * rows, :], d2d_send)
        bytes_of(oback, back_send)
        bytes_of(obuf.at[:, 0:nplane - 1], o_send)
        bytes_of(cbuf.at[0:nseq - 1, 0:1, :], cnt_send)
        bytes_of(statbuf.at[0:nseq - 1, 0:lead, :], st_send)
        bytes_of(wbuf.at[:, 0:(ntp - 1) * 64, :], w_send)
        bytes_of(wbuf.at[:, 0:(ntp - 1) * 64, :], wd_send)


def body(queries, keys, values, text_keys, text_values, prompt_lengths, frame_counts, out_weight):
    rows, width = queries.shape[1:]
    trows = text_keys.shape[1]
    heads = width // HD
    nseq, ntp = lax.axis_size("seq"), lax.axis_size("tp")
    model = out_weight.shape[1]
    cols = model // ntp
    keep = cols // 2
    wide = keep + 64
    vm = pl.BlockSpec(memory_space=pltpu.VMEM)
    sm = pl.BlockSpec(memory_space=pltpu.SMEM)
    hbm = pl.BlockSpec(memory_space=pl.ANY)
    dma = pltpu.SemaphoreType.DMA
    return pl.pallas_call(
        functools.partial(kernel, (heads, rows, trows, nseq, ntp, cols)),
        out_shape=jax.ShapeDtypeStruct((rows, keep), BF16),
        in_specs=[sm, sm, hbm, hbm, hbm, hbm, hbm, hbm],
        out_specs=vm,
        scratch_shapes=[
            pltpu.VMEM((rows, width), BF16),
            pltpu.VMEM((rows, width), BF16),
            pltpu.VMEM((trows, width), BF16),
            pltpu.VMEM((trows, width), BF16),
            pltpu.VMEM((8, HD), F32),
            pltpu.VMEM((3, rows, HD), BF16),
            pltpu.VMEM((3, 2, rows, HD), BF16),
            pltpu.VMEM((4, rows, HD), BF16),
            pltpu.VMEM((rows, HD), BF16),
            pltpu.VMEM((2, nseq * rows, HD), BF16),
            pltpu.VMEM((2, nseq * rows, HD), BF16),
            pltpu.VMEM((nseq * rows, HD), BF16),
            pltpu.VMEM((nseq * rows, HD), BF16),
            pltpu.VMEM((2, 2, trows, HD), BF16),
            pltpu.VMEM((trows, HD), BF16),
            pltpu.VMEM((nseq, 8, HD), F32),
            pltpu.VMEM((5, rows, HD), F32),
            pltpu.VMEM((5, rows, 2 * HD), F32),
            pltpu.VMEM((3, rows, HD), BF16),
            pltpu.VMEM((heads, 2 * ntp, rows, HD), BF16),
            pltpu.VMEM((heads, ntp * HD, wide), BF16),
            pltpu.VMEM((2, rows, wide), F32),
            pltpu.VMEM((16, HD), F32),
            pltpu.VMEM((nseq, 16, HD), F32),
            dma, dma((3,)), dma, dma((3,)), dma((4,)), dma, dma((4,)), dma((4,)),
            dma, dma((4, 4)), dma, dma((2, 8)), dma, dma, dma, dma((3,)),
            dma, dma((heads, 7)), dma, dma, dma, dma, dma, dma((9,)),
            dma, dma,
        ],
        compiler_params=pltpu.CompilerParams(
            collective_id=0, has_side_effects=True, vmem_limit_bytes=60 * 1024 * 1024
        ),
    )(
        prompt_lengths, frame_counts, queries[0], keys[0], values[0],
        text_keys[0], text_values[0], out_weight.reshape(heads, HD, model),
    )


def solution(mesh):
    placed = (
        P("cfg", "seq", "tp"),
        P("cfg", "seq", "tp"),
        P("cfg", "seq", "tp"),
        P("cfg", None, "tp"),
        P("cfg", None, "tp"),
        P("cfg"),
        P("seq"),
        P("tp", None),
    )
    return jax.shard_map(
        body, mesh=mesh, in_specs=placed, out_specs=P("seq", ("tp", "cfg")), check_vma=False
    )
```
